256 devices in a mesh: dp: 32 (over y, z), tensor: 8 (over x, core).
Axes of the slice: x: 4, y: 4, z: 8, core: 2. Of those that a mesh axis runs over, the one named last changes fastest.
Arguments:
- query: bfloat16 [256, 64, 128], P('dp', 'tensor'), may hold values from -8 to 8
- kv_pages: bfloat16 [2816, 8, 2, 128, 128], P('dp', 'tensor'), may hold values from -8 to 8
- move_plan: int32 [32, 3, 48], P('dp'), may hold values from 0 to 87, as said below
- move_count: int32 [32], P('dp'), may hold values from 36 to 48
- block_table: int32 [256, 8], P('dp'), may hold values from 0 to 87, as said below
- seq_lens: int32 [256], P('dp'), may hold values from 1 to 1024
- out_weight: bfloat16 [8192, 8192], P('tensor', 'dp'), may hold values from -0.0625 to 0.0625
Outputs:
- new_pages: bfloat16 [2816, 8, 2, 128, 128], P('dp', 'tensor')
- projected: bfloat16 [256, 8192], P(None, 'dp')
The draws below stay inside these ranges and needn't reach their ends.
Inputs may be any that keep to these rules, and one draw needn't show every extreme that they name: `move_plan`: row 0 holds the device's own source slots, distinct within a device; row 1 target devices; row 2 target slots. Entries at or past the device's move_count are padding to be ignored. At most 2 valid moves go from one device to one device, and some pair has exactly 2. The (target device, target slot) pairs of all valid moves are distinct. `block_table`: all entries of the sequences of one device are distinct slots of that device; sequence s belongs to device s // 8.
All inputs are finite; a program needn't handle non-finite values.
Results may differ from the reference program's by a relative error of at most 0.0055.
Values may be sent and summed in bfloat16 or wider, within the bound.
A program may use at most 64 MiB of HBM per device.

```python
import math
import jax
import jax.numpy as jnp
from jax import lax

D = 8192
HQ = 64
KVH = 8
HD = 128
BLOCK = 128
BLOCKS = 8
CAP = 2
SEQ_DEV = 8
MOVES = 48
SLOTS = 88
SEQS = 256
TOTAL_SLOTS = 2816
N_DP = 32


def derive(key, number):
    return jax.random.fold_in(key, number)


def move_layout(key):
    frequent_pages = jax.random.permutation(derive(key, 101), N_DP)[:2]
    extra_increment = jnp.zeros((N_DP,), jnp.int32).at[frequent_pages].set(2 ** 19)
    random_perturbation = jax.random.randint(derive(key, 102), (N_DP, N_DP), 0, 2 ** 20)
    order_ranks = (random_perturbation + extra_increment[None, :]) * N_DP + jnp.arange(N_DP, dtype=jnp.int32)[None, :]
    chosen = jnp.argsort(-order_ranks, axis=1, stable=True)[:, :MOVES // CAP]
    target_dev = jnp.repeat(chosen, CAP, axis=1).astype(jnp.int32)
    live_moves = jax.random.randint(derive(key, 103), (N_DP,), 3 * MOVES // 4, MOVES + 1).astype(jnp.int32)
    is_valid = jnp.arange(MOVES, dtype=jnp.int32)[None, :] < live_moves[:, None]
    slot_index = jnp.arange(SLOTS, dtype=jnp.int32)[None, :]
    source_key = jax.random.randint(derive(key, 104), (N_DP, SLOTS), 0, 2 ** 20) * SLOTS + slot_index
    source_slot = jnp.argsort(source_key, axis=1, stable=True)[:, :MOVES].astype(jnp.int32)
    shuffle_key = jax.random.randint(derive(key, 105), (N_DP, SLOTS), 0, 2 ** 20) * SLOTS + slot_index
    shuffled = jnp.argsort(shuffle_key, axis=1, stable=True).astype(jnp.int32)
    external_pages = (slot_index >= SEQ_DEV * BLOCKS).astype(jnp.int32)
    priority = (jax.random.randint(derive(key, 106), (N_DP, SLOTS), 0, 2 ** 20) + external_pages * 2 ** 21) * SLOTS + slot_index
    fill_order = jnp.argsort(priority, axis=1, stable=True)
    target_list = jnp.take_along_axis(shuffled, fill_order, axis=1)
    flat_dev = target_dev.reshape(-1)
    onehot = ((flat_dev[:, None] == jnp.arange(N_DP, dtype=jnp.int32)[None, :]) & is_valid.reshape(-1)[:, None]).astype(jnp.int32)
    before = jnp.cumsum(onehot, axis=0) - onehot
    dest_rank = jnp.sum(before * onehot, axis=1)
    target_slot = target_list[flat_dev, dest_rank].reshape(N_DP, MOVES)
    filler = jax.random.randint(derive(key, 107), (N_DP, MOVES), 0, SLOTS).astype(jnp.int32)
    target_slot = jnp.where(is_valid, target_slot, filler)
    move_plan = jnp.stack([source_slot, target_dev, target_slot], axis=1).astype(jnp.int32)
    page_table = shuffled[:, :SEQ_DEV * BLOCKS].reshape(N_DP * SEQ_DEV, BLOCKS).astype(jnp.int32)
    return (move_plan, live_moves, page_table)


def draw_move_plan(key, part):
    return move_layout(key)[0]


def draw_move_count(key, part):
    return move_layout(key)[1]


def draw_block_table(key, part):
    return move_layout(key)[2]


def draw_query(key, part):
    shape = (SEQS, HQ, HD)
    values = jnp.clip(jax.random.normal(derive(key, 14), shape, jnp.float32), -6.0, 6.0)
    return values.astype(jnp.bfloat16)


def draw_kv_pages(key, part):
    shape = (TOTAL_SLOTS, KVH, 2, BLOCK, HD)
    values = jnp.clip(jax.random.normal(derive(key, 24), shape, jnp.float32), -6.0, 6.0)
    return values.astype(jnp.bfloat16)


def set_ends(entries, rng, smallest, high):
    place = [jax.random.randint(jax.random.fold_in(rng, axis), (), 0, length) for axis, length in enumerate(entries.shape)]
    widest = entries.shape.index(max(entries.shape))
    next_to = place[:widest] + [(place[widest] + 1) % entries.shape[widest]] + place[widest + 1:]
    return entries.at[tuple(place)].set(smallest).at[tuple(next_to)].set(high)


def level_of(rng, extent, shards, least, top_value):
    factor_of = 1.0
    for axis_at, blocks in shards:
        heights = jax.random.uniform(jax.random.fold_in(jax.random.fold_in(rng, 6), axis_at), (blocks,), jnp.float32, least / len(shards), top_value / len(shards))
        factor_of = factor_of * jnp.repeat(jnp.exp(heights), extent[axis_at] // blocks).reshape((-1,) + (1,) * (len(extent) - 1 - axis_at))
    return factor_of


def normal_values(rng, shape, scale, most, split=(), kind=jnp.bfloat16):
    drawn = jax.random.normal(rng, shape, jnp.float32) * scale
    if len(split) > 0:
        drawn = level_of(rng, shape, split, -0.22, 0.18) * drawn
    return jnp.clip(drawn, min=-most, max=most).astype(kind)


def setup_inputs(seed: int = 0) -> dict:
    key_list = jax.random.split(jax.random.key(seed), 8)
    return {
        "query": draw_query(jax.random.fold_in(key_list[7], 71), 0),
        "kv_pages": draw_kv_pages(jax.random.fold_in(key_list[7], 71), 0),
        "move_plan": draw_move_plan(jax.random.fold_in(key_list[7], 71), 0),
        "move_count": draw_move_count(jax.random.fold_in(key_list[7], 71), 0),
        "block_table": draw_block_table(jax.random.fold_in(key_list[7], 71), 0),
        "seq_lens": set_ends(jax.random.randint(key_list[5], (SEQS,), 1, BLOCKS * BLOCK + 1), jax.random.fold_in(key_list[5], 1), 1, BLOCKS * BLOCK).astype(jnp.int32),
        "out_weight": normal_values(key_list[6], (HQ * HD, D), (HQ * HD) ** -0.5, 0.0625, ((0, 8), (1, 32))),
    }


def reference(query, kv_pages, move_plan, move_count, block_table, seq_lens, out_weight):
    sender = jnp.arange(N_DP, dtype=jnp.int32)[:, None]
    is_valid = jnp.arange(MOVES, dtype=jnp.int32)[None, :] < move_count[:, None]
    source = (sender * SLOTS + move_plan[:, 0, :]).reshape(-1).astype(jnp.int32)
    target = jnp.where(is_valid, move_plan[:, 1, :] * SLOTS + move_plan[:, 2, :], TOTAL_SLOTS)
    target = target.reshape(-1).astype(jnp.int32)
    new_pages = kv_pages.at[target].set(kv_pages[source], mode='drop')
    owner_dev = jnp.arange(SEQS, dtype=jnp.int32) // SEQ_DEV
    page_slots = (owner_dev[:, None] * SLOTS + block_table).astype(jnp.int32)
    position = jnp.arange(BLOCKS * BLOCK, dtype=jnp.int32)
    score_scale = 1.0 / math.sqrt(HD)

    def attend(inputs):
        query_row, rows_used, length = inputs
        gathered = new_pages[rows_used]
        key_rows = jnp.transpose(gathered[:, :, 0], (1, 0, 2, 3)).reshape(KVH, BLOCKS * BLOCK, HD).astype(jnp.float32)
        value_rows = jnp.transpose(gathered[:, :, 1], (1, 0, 2, 3)).reshape(KVH, BLOCKS * BLOCK, HD).astype(jnp.float32)
        grouped = query_row.reshape(KVH, HQ // KVH, HD).astype(jnp.float32)
        scores = jnp.einsum('kgd,ktd->kgt', grouped, key_rows) * score_scale
        scores = jnp.where(position[None, None, :] < length, scores, -1e+30)
        largest = lax.optimization_barrier(jnp.max(scores, axis=-1, keepdims=True))
        expo = jnp.exp(scores - largest)
        weights = (expo / lax.optimization_barrier(jnp.sum(expo, axis=-1, keepdims=True))).astype(jnp.bfloat16)
        mixed_heads = jnp.einsum('kgt,ktd->kgd', weights.astype(jnp.float32), value_rows)
        return mixed_heads.reshape(HQ * HD).astype(jnp.bfloat16)
    attention = lax.map(attend, (query, page_slots, seq_lens))
    projected = jnp.dot(attention, out_weight, preferred_element_type=jnp.float32).astype(jnp.bfloat16)
    return (new_pages, projected)
```

```python
import functools
import math

import jax
import jax.numpy as jnp
from jax import lax
from jax.experimental import pallas as pl
from jax.experimental.pallas import tpu as pltpu
from jax.sharding import PartitionSpec as P

HD = 128
BLOCK = 128
BLOCKS = 8
CAP = 2
SLOTS = 88
MOVES = 48
NY, NZ = 4, 8
NDP = NY * NZ
NT = 8
SEQ_DEV = 8
MESH = pl.DeviceIdType.MESH
VMEM_LIMIT = 60 * 1024 * 1024
PAGE = (2, BLOCK, HD)
SHIFTS = [(dy, dz) for dy in range(NY) for dz in range(NZ)]


def far(shift):
    return min(shift[0], NY - shift[0]) + min(shift[1], NZ - shift[1])


def vspec():
    return pl.BlockSpec(memory_space=pltpu.VMEM)


def sspec():
    return pl.BlockSpec(memory_space=pltpu.SMEM)


def aspec():
    return pl.BlockSpec(memory_space=pl.ANY)


def pack_kernel(plan_ref, count_ref, kv_ref, send_ref, tags_ref, used, sems):
    me = lax.axis_index("dp")
    y, z = me // NZ, me % NZ
    for k in range(NDP):
        used[k] = 0
    count = count_ref[0]
    rows = lax.broadcasted_iota(jnp.int32, (NDP, 128), 0)
    cols = lax.broadcasted_iota(jnp.int32, (NDP, 128), 1)

    def step(m, tags):
        valid = m < count
        target = plan_ref[1, m]
        shift = lax.rem(target // NZ - y + NY, NY) * NZ + lax.rem(target % NZ - z + NZ, NZ)
        rank = used[shift]

        @pl.when(valid)
        def _():
            used[shift] = rank + 1
            pltpu.make_async_copy(
                kv_ref.at[plan_ref[0, m]], send_ref.at[shift * CAP + rank], sems.at[m]
            ).start()

        hit = (rows == shift) & (cols == rank) & valid
        return jnp.where(hit, plan_ref[2, m], tags)

    tags = lax.fori_loop(0, MOVES, step, jnp.full((NDP, 128), -1, jnp.int32))
    tags_ref[...] = tags.reshape(NDP, 1, 128)

    def drain(m, carry):
        @pl.when(m < count)
        def _():
            pltpu.make_async_copy(kv_ref.at[0], send_ref.at[0], sems.at[m]).wait()

        return carry

    lax.fori_loop(0, MOVES, drain, 0)


def exchange_kernel(send_ref, tags_ref, kv_ref, comb_ref, got_ref, load_sem, send_sem, recv_sem, tag_send, tag_recv):
    me = lax.axis_index("dp")
    t = lax.axis_index("tensor")
    y, z = me // NZ, me % NZ
    load = pltpu.make_async_copy(kv_ref, comb_ref.at[pl.ds(0, SLOTS)], load_sem)
    load.start()
    bar = pltpu.get_barrier_semaphore()
    order = sorted([s for s in SHIFTS if s != (0, 0)], key=lambda s: -far(s))
    peer = {}
    for dy, dz in order:
        peer[dy, dz] = lax.rem(y + dy, NY) * NZ + lax.rem(z + dz, NZ)
        pl.semaphore_signal(bar, inc=1, device_id=(peer[dy, dz], t), device_id_type=MESH)
    pl.semaphore_wait(bar, len(order))
    copies = []
    for dy, dz in order:
        k = dy * NZ + dz
        copy = pltpu.make_async_remote_copy(
            src_ref=send_ref.at[pl.ds(k * CAP, CAP)],
            dst_ref=comb_ref.at[pl.ds(SLOTS + k * CAP, CAP)],
            send_sem=send_sem.at[k],
            recv_sem=recv_sem.at[k],
            device_id=(peer[dy, dz], t),
            device_id_type=MESH,
        )
        copy.start()
        copies.append(copy)
        copy = pltpu.make_async_remote_copy(
            src_ref=tags_ref.at[k],
            dst_ref=got_ref.at[k],
            send_sem=tag_send.at[k],
            recv_sem=tag_recv.at[k],
            device_id=(peer[dy, dz], t),
            device_id_type=MESH,
        )
        copy.start()
        copies.append(copy)
    got_ref[0] = tags_ref[0]
    comb_ref[SLOTS : SLOTS + CAP] = send_ref[0:CAP]
    load.wait()
    for copy in copies:
        copy.wait()


def attend_kernel(got_ref, table_ref, lens_ref, query_ref, comb_ref, new_ref, att_ref, where_ref, mixed, sems):
    for s in range(SLOTS):
        where_ref[s] = s
    for k in range(NDP):
        for c in range(CAP):
            slot = got_ref[k, c]

            @pl.when(slot >= 0)
            def _():
                where_ref[slot] = SLOTS + k * CAP + c

    copies = []
    for s in range(SLOTS):
        copy = pltpu.make_async_copy(comb_ref.at[where_ref[s]], new_ref.at[s], sems.at[s])
        copy.start()
        copies.append(copy)
    position = lax.broadcasted_iota(jnp.int32, (8, BLOCKS * BLOCK), 1)
    for s in range(SEQ_DEV):
        at = [where_ref[table_ref[s, b]] for b in range(BLOCKS)]
        keys = jnp.concatenate([comb_ref[i, 0] for i in at], axis=0)
        scores = lax.dot_general(
            query_ref[s], keys, (((1,), (1,)), ((), ())), preferred_element_type=jnp.float32
        ) * (1.0 / math.sqrt(HD))
        scores = jnp.where(position < lens_ref[s], scores, -1e30)
        expo = jnp.exp(scores - jnp.max(scores, axis=1, keepdims=True))
        weights = (expo / jnp.sum(expo, axis=1, keepdims=True)).astype(jnp.bfloat16)
        values = jnp.concatenate([comb_ref[i, 1] for i in at], axis=0)
        mixed[s * 8 : s * 8 + 8, :] = jnp.dot(weights, values, preferred_element_type=jnp.float32)
    att_ref[...] = jnp.concatenate(
        [mixed[pl.ds(h, SEQ_DEV, stride=8), :] for h in range(8)], axis=1
    ).astype(jnp.bfloat16)
    for copy in copies:
        copy.wait()


def project_kernel(att_ref, w_ref, out_ref, gath, part, red, z_send, z_recv, y_send, y_recv, r_send, r_recv, o_send, o_recv):
    me = lax.axis_index("dp")
    t = lax.axis_index("tensor")
    y, z = me // NZ, me % NZ
    zs = [lax.rem(z + d, NZ) for d in range(NZ)]
    ys = [lax.rem(y + d, NY) for d in range(NY)]
    ts = [lax.rem(t + d, NT) for d in range(NT)]
    bar = pltpu.get_barrier_semaphore()
    peers = (
        [(y * NZ + zs[d], t) for d in range(1, NZ)]
        + [(ys[d] * NZ + z, t) for d in range(1, NY)]
        + [(me, ts[d]) for d in range(1, NT)]
    )
    for peer in peers:
        pl.semaphore_signal(bar, inc=1, device_id=peer, device_id_type=MESH)
    pl.semaphore_wait(bar, len(peers))

    def remote(src, dst, send, recv, device):
        copy = pltpu.make_async_remote_copy(
            src_ref=src, dst_ref=dst, send_sem=send, recv_sem=recv, device_id=device, device_id_type=MESH
        )
        copy.start()
        return copy

    z_order = sorted(range(1, NZ), key=lambda d: -min(d, NZ - d))
    along_z = {d: remote(att_ref, gath.at[me], z_send.at[d], z_recv.at[d], (y * NZ + zs[d], t)) for d in z_order}
    gath[me] = att_ref[...]
    along_y = []
    for d in range(1, NY):
        along_y.append(remote(att_ref, gath.at[me], y_send.at[d], y_recv.at[d], (ys[d] * NZ + z, t)))
    for e in sorted(range(1, NZ), key=lambda d: min(d, NZ - d)):
        along_z[e].wait_recv()
        held = y * NZ + lax.rem(z - e + NZ, NZ)
        for d in (2, 1, 3):
            n = e * NY + d
            along_y.append(remote(gath.at[held], gath.at[held], y_send.at[n], y_recv.at[n], (ys[d] * NZ + z, t)))
    for copy in along_y:
        copy.wait_recv()
    rows = gath[...].reshape(NDP * SEQ_DEV, 8 * HD)
    part[...] = jnp.dot(rows, w_ref[...], preferred_element_type=jnp.float32)
    chunk = NDP * SEQ_DEV // NT
    t_order = (4, 5, 3, 2, 6, 1, 7)

    def rows_of(i):
        return pl.ds(pl.multiple_of(i * chunk, chunk), chunk)

    sums = [remote(part.at[rows_of(ts[d])], red.at[d], r_send.at[d], r_recv.at[d], (me, ts[d])) for d in t_order]
    total = part[rows_of(t), :]
    for copy in sums:
        copy.wait_recv()
    for d in range(1, NT):
        total = total + red[d]
    out_ref[rows_of(t), :] = total.astype(jnp.bfloat16)
    outs = [
        remote(out_ref.at[rows_of(t)], out_ref.at[rows_of(t)], o_send.at[d], o_recv.at[d], (me, ts[d])) for d in t_order
    ]
    for copy in outs:
        copy.wait_recv()
    for d in range(1, NZ):
        along_z[d].wait_send()
    for copy in along_y + sums + outs:
        copy.wait_send()


def body(query, kv_pages, move_plan, move_count, block_table, seq_lens, out_weight):
    kv = kv_pages.reshape(SLOTS, *PAGE)
    dma = pltpu.SemaphoreType.DMA
    send, tags = pl.pallas_call(
        pack_kernel,
        name="pack",
        out_shape=[pltpu.VMEM((NDP * CAP, *PAGE), jnp.bfloat16), pltpu.VMEM((NDP, 1, 128), jnp.int32)],
        in_specs=[sspec(), sspec(), aspec()],
        out_specs=[vspec(), vspec()],
        scratch_shapes=[pltpu.SMEM((NDP,), jnp.int32), dma((MOVES,))],
        compiler_params=pltpu.CompilerParams(vmem_limit_bytes=VMEM_LIMIT // 2),
    )(move_plan[0], move_count, kv)
    comb, got = pl.pallas_call(
        exchange_kernel,
        name="exchange",
        out_shape=[pltpu.VMEM((SLOTS + NDP * CAP, *PAGE), jnp.bfloat16), pltpu.VMEM((NDP, 1, 128), jnp.int32)],
        in_specs=[vspec(), vspec(), aspec()],
        out_specs=[vspec(), vspec()],
        scratch_shapes=[dma(()), dma((NDP,)), dma((NDP,)), dma((NDP,)), dma((NDP,))],
        compiler_params=pltpu.CompilerParams(
            collective_id=0, has_side_effects=True, vmem_limit_bytes=VMEM_LIMIT // 2
        ),
    )(send, tags, kv)
    new_pages, attention = pl.pallas_call(
        attend_kernel,
        name="attend",
        out_shape=[
            jax.ShapeDtypeStruct((SLOTS, *PAGE), jnp.bfloat16),
            pltpu.VMEM((SEQ_DEV, 8 * HD), jnp.bfloat16),
        ],
        in_specs=[sspec(), sspec(), sspec(), vspec(), vspec()],
        out_specs=[aspec(), vspec()],
        scratch_shapes=[pltpu.SMEM((SLOTS,), jnp.int32), pltpu.VMEM((64, HD), jnp.float32), dma((SLOTS,))],
        compiler_params=pltpu.CompilerParams(vmem_limit_bytes=VMEM_LIMIT // 2),
    )(got.reshape(NDP, 128), block_table, seq_lens, query, comb)
    projected = pl.pallas_call(
        project_kernel,
        name="project",
        out_shape=jax.ShapeDtypeStruct((NDP * SEQ_DEV, out_weight.shape[1]), jnp.bfloat16),
        in_specs=[vspec(), vspec()],
        out_specs=vspec(),
        scratch_shapes=[
            pltpu.VMEM((NDP, SEQ_DEV, 8 * HD), jnp.bfloat16),
            pltpu.VMEM((NDP * SEQ_DEV, 256), jnp.float32),
            pltpu.VMEM((NT, NDP * SEQ_DEV // NT, 256), jnp.float32),
            dma((NZ,)), dma((NZ,)), dma((NDP,)), dma((NDP,)), dma((NT,)), dma((NT,)), dma((NT,)), dma((NT,)),
        ],
        compiler_params=pltpu.CompilerParams(
            collective_id=1, has_side_effects=True, vmem_limit_bytes=VMEM_LIMIT // 2
        ),
    )(attention, out_weight)
    return new_pages.reshape(kv_pages.shape), projected


def solution(mesh):
    placed = (
        P("dp", "tensor", None),
        P("dp", "tensor", None, None, None),
        P("dp", None, None),
        P("dp"),
        P("dp", None),
        P("dp"),
        P("tensor", "dp"),
    )
    return jax.shard_map(
        body,
        mesh=mesh,
        in_specs=placed,
        out_specs=(P("dp", "tensor", None, None, None), P(None, "dp")),
        check_vma=False,
    )
```

```python
import functools
import math

import jax
import jax.numpy as jnp
from jax import lax
from jax.experimental import pallas as pl
from jax.experimental.pallas import tpu as pltpu
from jax.sharding import PartitionSpec as P

HD = 128
BLOCK = 128
BLOCKS = 8
CAP = 2
SLOTS = 88
MOVES = 48
NY, NZ = 4, 8
NDP = NY * NZ
NT = 8
SEQ_DEV = 8
HEADS = 8
WINDOW = 8
NEG = -1e30
SCALE = 1.0 / math.sqrt(HD)
MESH = pl.DeviceIdType.MESH
VMEM_LIMIT = 16 * 1024 * 1024
PAGE = (2, BLOCK, HD)
SHIFTS = [(dy, dz) for dy in range(NY) for dz in range(NZ)]
f32 = jnp.float32
bf16 = jnp.bfloat16


def far(shift):
    return min(shift[0], NY - shift[0]) + min(shift[1], NZ - shift[1])


def vspec():
    return pl.BlockSpec(memory_space=pltpu.VMEM)


def sspec():
    return pl.BlockSpec(memory_space=pltpu.SMEM)


def hspec():
    return pl.BlockSpec(memory_space=pltpu.HBM)


def pack_kernel(plan_ref, count_ref, table_ref, lens_ref, kv_ref, send_ref, tags_ref, meta_ref, used, sems):
    me = lax.axis_index("dp")
    y, z = me // NZ, me % NZ
    for k in range(NDP):
        used[k] = 0
    count = count_ref[0]
    rows = lax.broadcasted_iota(jnp.int32, (NDP, 128), 0)
    cols = lax.broadcasted_iota(jnp.int32, (NDP, 128), 1)

    def step(m, tags):
        valid = m < count
        target = plan_ref[1, 0, m]
        shift = lax.rem(target // NZ - y + NY, NY) * NZ + lax.rem(target % NZ - z + NZ, NZ)
        rank = used[shift]

        @pl.when(valid)
        def _():
            used[shift] = rank + 1
            pltpu.make_async_copy(
                kv_ref.at[plan_ref[0, 0, m]], send_ref.at[shift * CAP + rank], sems.at[m]
            ).start()

        hit = (rows == shift) & (cols == rank) & valid
        return jnp.where(hit, plan_ref[2, 0, m], tags)

    tags = lax.fori_loop(0, MOVES, step, jnp.full((NDP, 128), -1, jnp.int32))
    tags_ref[...] = tags.reshape(NDP, 1, 128)
    lane = lax.broadcasted_iota(jnp.int32, (1, 128), 1)
    meta = jnp.full((1, 128), -2, jnp.int32)
    for s in range(SEQ_DEV):
        for b in range(BLOCKS):
            meta = jnp.where(lane == s * BLOCKS + b, table_ref[s, b], meta)
        meta = jnp.where(lane == SEQ_DEV * BLOCKS + s, lens_ref[s], meta)
    meta_ref[0] = meta

    def drain(m, carry):
        @pl.when(m < count)
        def _():
            pltpu.make_async_copy(kv_ref.at[0], send_ref.at[0], sems.at[m]).wait()

        return carry

    lax.fori_loop(0, MOVES, drain, 0)


def step_kernel(
    table_ref, lens_ref, send_ref, tags_ref, meta_ref, query_ref, w_ref, kv_ref,
    local_ref, recv_ref, code_ref, out_ref,
    got, metas, qall, src_seq, src_end, arr_seq, part, lse, apart, alse, wide, mixed, att, gath, proj, red,
    load_sem, page_send, page_recv, tag_sem, meta_sem, part_sem, lse_sem,
    qz_send, qz_recv, qy_send, qy_recv, z_send, z_recv, y_send, y_recv, r_send, r_recv, o_send, o_recv,
):
    me = lax.axis_index("dp")
    t = lax.axis_index("tensor")
    y, z = me // NZ, me % NZ
    zs = [lax.rem(z + d, NZ) for d in range(NZ)]
    ys = [lax.rem(y + d, NY) for d in range(NY)]
    ts = [lax.rem(t + d, NT) for d in range(NT)]
    load = pltpu.make_async_copy(kv_ref, local_ref, load_sem)
    load.start()
    bar = pltpu.get_barrier_semaphore()
    order = sorted([s for s in SHIFTS if s != (0, 0)], key=lambda s: -far(s))
    peers = [(ys[dy] * NZ + zs[dz], t) for dy, dz in order] + [(me, ts[d]) for d in range(1, NT)]
    for peer in peers:
        pl.semaphore_signal(bar, inc=1, device_id=peer, device_id_type=MESH)
    pl.semaphore_wait(bar, len(peers))

    def remote(src, dst, send, recv, device):
        copy = pltpu.make_async_remote_copy(
            src_ref=src, dst_ref=dst, send_sem=send, recv_sem=recv, device_id=device, device_id_type=MESH
        )
        copy.start()
        return copy

    def to(shift):
        return (ys[shift[0]] * NZ + zs[shift[1]], t)

    def at(shift):
        return shift[0] * NZ + shift[1]

    pages = []
    pending = [(c, s) for c in range(CAP) for s in order]

    def pump(n):
        for _ in range(n):
            i = len(pages)
            if i >= len(pending):
                return
            if i >= WINDOW:
                pages[i - WINDOW].wait_send()
            c, s = pending[i]
            row = at(s) * CAP + c
            pages.append(
                remote(send_ref.at[row], recv_ref.at[row], page_send.at[i % WINDOW], page_recv.at[0], to(s))
            )

    z_order = sorted(range(1, NZ), key=lambda d: -min(d, NZ - d))
    z_near = sorted(range(1, NZ), key=lambda d: min(d, NZ - d))

    def gather_start(own_ref, buf, zsend, zrecv, ysend, yrecv):
        along_z = {d: remote(own_ref, buf.at[me], zsend.at[d], zrecv.at[d], (y * NZ + zs[d], t)) for d in z_order}
        along_y = [
            remote(own_ref, buf.at[me], ysend.at[d], yrecv.at[d], (ys[d] * NZ + z, t)) for d in (2, 1, 3)
        ]
        buf[me] = own_ref[...]
        return along_z, along_y

    def gather_forward(along_z, along_y, buf, ysend, yrecv, pumps):
        for e in z_near:
            along_z[e].wait_recv()
            held = y * NZ + lax.rem(z - e + NZ, NZ)
            for d in (2, 1, 3):
                n = e * NY + d
                along_y.append(
                    remote(buf.at[held], buf.at[held], ysend.at[n], yrecv.at[n], (ys[d] * NZ + z, t))
                )
            pump(pumps)

    q_z, q_y = gather_start(query_ref, qall, qz_send, qz_recv, qy_send, qy_recv)
    small = []
    for s in order:
        back = ((NY - s[0]) % NY, (NZ - s[1]) % NZ)
        small.append(remote(tags_ref.at[at(s)], got.at[at(s)], tag_sem.at[0], tag_sem.at[1], to(s)))
        small.append(remote(meta_ref.at[0], metas.at[at(back)], meta_sem.at[0], meta_sem.at[1], to(s)))
    got[0] = tags_ref[0]
    metas[0] = meta_ref[0]
    pump(WINDOW)
    recv_ref[0:CAP] = send_ref[0:CAP]
    gather_forward(q_z, q_y, qall, qy_send, qy_recv, 1)

    def all_of(buf, sems):
        return pltpu.make_async_remote_copy(
            src_ref=buf.at[pl.ds(1, NDP - 1)],
            dst_ref=buf.at[pl.ds(1, NDP - 1)],
            send_sem=sems.at[0],
            recv_sem=sems.at[1],
            device_id=(me, ts[1]),
            device_id_type=MESH,
        )

    all_of(got, tag_sem).wait_recv()
    all_of(metas, meta_sem).wait_recv()
    lane = lax.broadcasted_iota(jnp.int32, (NDP, 128), 1)
    lane_f = lane.astype(f32)
    first = lane < SEQ_DEV * BLOCKS
    seq_f = (lane // BLOCKS).astype(f32)
    block_f = (lane % BLOCKS).astype(f32)
    device_f = lax.broadcasted_iota(jnp.int32, (NDP, 128), 0).astype(f32)
    mine = metas[0]
    moved = jnp.zeros((1, 128), f32)
    code = jnp.zeros((1, 128), f32)
    sent_tags = tags_ref[...].reshape(NDP, 128)
    got_tags = got[...].reshape(NDP, 128)
    tables = metas[...].reshape(NDP, 128)

    def spread(column):
        return jnp.broadcast_to(column, (NDP, 128)).reshape(NDP, 1, 128)

    for c in range(CAP):
        tag = sent_tags[:, c : c + 1]
        hit = (tables == tag) & first & (tag >= 0)
        found = jnp.sum(jnp.where(hit, 1.0, 0.0), axis=1, keepdims=True)
        seq = jnp.sum(jnp.where(hit, seq_f, 0.0), axis=1, keepdims=True)
        block = jnp.sum(jnp.where(hit, block_f, 0.0), axis=1, keepdims=True)
        ends = jnp.sum(
            jnp.where(lane_f == seq + SEQ_DEV * BLOCKS, tables.astype(f32), 0.0), axis=1, keepdims=True
        )
        src_seq[c] = spread(jnp.where(found > 0, seq, -1.0))
        src_end[c] = spread(ends - block * BLOCK)
        tag = got_tags[:, c : c + 1]
        hit = (mine == tag) & first & (tag >= 0)
        found = jnp.sum(jnp.where(hit, 1.0, 0.0), axis=1, keepdims=True)
        seq = jnp.sum(jnp.where(hit, seq_f, 0.0), axis=1, keepdims=True)
        arr_seq[c] = spread(jnp.where(found > 0, seq, -1.0))
        moved = jnp.maximum(moved, jnp.max(jnp.where(hit, 1.0, 0.0), axis=0, keepdims=True))
        code = code + jnp.sum(jnp.where(lane == tag, device_f * CAP + (c + 1), 0.0), axis=0, keepdims=True)
    code_ref[...] = code.astype(jnp.int32)
    pump(2)

    load.wait()
    position = lax.broadcasted_iota(jnp.int32, (HEADS, BLOCKS * BLOCK), 1)
    kept_o = []
    kept_lse = []
    for s in range(SEQ_DEV):
        index = [table_ref[s, b] for b in range(BLOCKS)]
        keys = jnp.concatenate([local_ref[i, 0] for i in index], axis=0)
        scores = lax.dot_general(
            query_ref[s * HEADS : (s + 1) * HEADS, :], keys, (((1,), (1,)), ((), ())), preferred_element_type=f32
        ) * SCALE
        gone = jnp.concatenate(
            [jnp.broadcast_to(moved[:, s * BLOCKS + b : s * BLOCKS + b + 1], (1, BLOCK)) for b in range(BLOCKS)], axis=1
        )
        scores = jnp.where((position < lens_ref[s]) & (gone == 0), scores, NEG)
        largest = jnp.max(scores, axis=1, keepdims=True)
        expo = jnp.exp(scores - largest)
        total = jnp.sum(expo, axis=1, keepdims=True)
        values = jnp.concatenate([local_ref[i, 1] for i in index], axis=0)
        mixed[s * HEADS : (s + 1) * HEADS, :] = (
            jnp.dot(expo.astype(bf16), values, preferred_element_type=f32) / total
        )
        wide[s] = jnp.broadcast_to(largest + jnp.log(total), (HEADS, 128))
        if s % 2:
            pump(1)

    for copy in q_y:
        copy.wait_recv()
    lane8 = lax.broadcasted_iota(jnp.int32, (HEADS, 128), 1)
    row8 = lax.broadcasted_iota(jnp.int32, (HEADS, 128), 0)
    lane8_f = lane8.astype(f32)

    def rows8(ref, c, k):
        return jnp.broadcast_to(ref[c, k], (HEADS, 128))

    def partial(k, carry):
        dy, dz = k // NZ, lax.rem(k, NZ)
        owner = lax.rem(y + dy, NY) * NZ + lax.rem(z + dz, NZ)
        asked = qall[owner]
        keys = jnp.concatenate([send_ref[k * CAP + c, 0] for c in range(CAP)], axis=0)
        every = lax.dot_general(asked, keys, (((1,), (1,)), ((), ())), preferred_element_type=f32) * SCALE
        row = jnp.zeros((1, 128), f32)
        for c in range(CAP):
            seq = rows8(src_seq, c, k)
            scores = jnp.full((HEADS, BLOCK), NEG, f32)
            for s in range(SEQ_DEV):
                scores = jnp.where(
                    seq == s, every[s * HEADS : (s + 1) * HEADS, c * BLOCK : (c + 1) * BLOCK], scores
                )
            scores = jnp.where(lane8_f < rows8(src_end, c, k), scores, NEG)
            largest = jnp.max(scores, axis=1, keepdims=True)
            expo = jnp.exp(scores - largest)
            total = jnp.sum(expo, axis=1, keepdims=True)
            o = jnp.dot(expo.astype(bf16), send_ref[k * CAP + c, 1], preferred_element_type=f32) / total
            part[k, c] = jnp.where(seq >= 0, o, 0.0).astype(bf16)
            weight = jnp.where(seq >= 0, largest + jnp.log(total), NEG)
            row = row + jnp.sum(jnp.where(lane8 == row8 + c * HEADS, weight, 0.0), axis=0, keepdims=True)
        lse[k] = row
        return carry

    for g in range(4):
        lax.fori_loop(g * NZ, (g + 1) * NZ, partial, 0)
        for dz in range(NZ):
            if (g, dz) != (0, 0):
                k = at((g, dz))
                small.append(remote(part.at[k], apart.at[k], part_sem.at[0], part_sem.at[1], to((g, dz))))
                small.append(remote(lse.at[k], alse.at[k], lse_sem.at[0], lse_sem.at[1], to((g, dz))))
        pump(2)
    apart[0] = part[0]
    alse[0] = lse[0]
    pump(3)
    all_of(apart, part_sem).wait_recv()
    all_of(alse, lse_sem).wait_recv()

    def widen(k, tops):
        tops = list(tops)
        for c in range(CAP):
            column = jnp.sum(
                jnp.where(lane8 == row8 + c * HEADS, jnp.broadcast_to(alse[k], (HEADS, 128)), 0.0),
                axis=1,
                keepdims=True,
            )
            full = jnp.broadcast_to(column, (HEADS, 128))
            wide[SEQ_DEV + k * CAP + c] = full
            seq = rows8(arr_seq, c, k)
            for s in range(SEQ_DEV):
                tops[s] = jnp.where(seq == s, jnp.maximum(tops[s], full), tops[s])
        return tuple(tops)

    tops = lax.fori_loop(0, NDP, widen, tuple(wide[s] for s in range(SEQ_DEV)))
    start = []
    for s in range(SEQ_DEV):
        w = jnp.exp(wide[s] - tops[s])
        start.append((w, w * mixed[s * HEADS : (s + 1) * HEADS, :]))

    def merge(k, sums):
        dens, nums = list(sums[0]), list(sums[1])
        for c in range(CAP):
            seq = rows8(arr_seq, c, k)
            top = jnp.zeros((HEADS, 128), f32)
            for s in range(SEQ_DEV):
                top = jnp.where(seq == s, tops[s], top)
            w = jnp.exp(wide[SEQ_DEV + k * CAP + c] - top)
            o = w * apart[k, c].astype(f32)
            for s in range(SEQ_DEV):
                dens[s] = jnp.where(seq == s, dens[s] + w, dens[s])
                nums[s] = jnp.where(seq == s, nums[s] + o, nums[s])
        return tuple(dens), tuple(nums)

    dens, nums = lax.fori_loop(
        0, NDP, merge, (tuple(a for a, _ in start), tuple(b for _, b in start))
    )
    for s in range(SEQ_DEV):
        mixed[s * HEADS : (s + 1) * HEADS, :] = nums[s] / dens[s]
    att[...] = jnp.concatenate(
        [mixed[pl.ds(h, SEQ_DEV, stride=HEADS), :] for h in range(HEADS)], axis=1
    ).astype(bf16)

    along_z, along_y = gather_start(att, gath, z_send, z_recv, y_send, y_recv)
    pump(4)
    gather_forward(along_z, along_y, gath, y_send, y_recv, 1)
    pump(2)
    for copy in along_y:
        copy.wait_recv()
    rows = gath[...].reshape(NDP * SEQ_DEV, HEADS * HD)
    proj[...] = jnp.dot(rows, w_ref[...], preferred_element_type=f32)
    chunk = NDP * SEQ_DEV // NT
    t_order = (4, 5, 3, 2, 6, 1, 7)

    def rows_of(i):
        return pl.ds(pl.multiple_of(i * chunk, chunk), chunk)

    sums = [remote(proj.at[rows_of(ts[d])], red.at[d], r_send.at[d], r_recv.at[d], (me, ts[d])) for d in t_order]
    pump(2)
    total = proj[rows_of(t), :]
    for copy in sums:
        copy.wait_recv()
    for d in range(1, NT):
        total = total + red[d]
    out_ref[rows_of(t), :] = total.astype(bf16)
    outs = [
        remote(out_ref.at[rows_of(t)], out_ref.at[rows_of(t)], o_send.at[d], o_recv.at[d], (me, ts[d])) for d in t_order
    ]
    pump(len(pending))
    for copy in outs:
        copy.wait_recv()
    for copy in pages[-WINDOW:]:
        copy.wait_send()
    for copy in list(q_z.values()) + q_y + list(along_z.values()) + along_y + sums + outs:
        copy.wait_send()
    all_of(got, tag_sem).wait_send()
    all_of(metas, meta_sem).wait_send()
    all_of(part, part_sem).wait_send()
    all_of(lse, lse_sem).wait_send()
    moved_pages = recv_ref.at[pl.ds(CAP, (NDP - 1) * CAP)]
    pltpu.make_async_remote_copy(
        src_ref=moved_pages, dst_ref=moved_pages, send_sem=page_send.at[0], recv_sem=page_recv.at[0],
        device_id=(me, ts[1]), device_id_type=MESH,
    ).wait_recv()


def place_kernel(code_ref, local_ref, recv_ref, proj_ref, new_ref, out_ref, sems, out_sem):
    result = pltpu.make_async_copy(proj_ref, out_ref, out_sem)
    result.start()

    def put(s, carry):
        code = code_ref[0, s]

        @pl.when(code == 0)
        def _():
            pltpu.make_async_copy(local_ref.at[s], new_ref.at[s], sems.at[s]).start()

        @pl.when(code > 0)
        def _():
            pltpu.make_async_copy(recv_ref.at[code - 1], new_ref.at[s], sems.at[s]).start()

        return carry

    lax.fori_loop(0, SLOTS, put, 0)

    def drain(s, carry):
        pltpu.make_async_copy(local_ref.at[0], new_ref.at[0], sems.at[s]).wait()
        return carry

    lax.fori_loop(0, SLOTS, drain, 0)
    result.wait()


def body(query, kv_pages, move_plan, move_count, block_table, seq_lens, out_weight):
    kv = kv_pages.reshape(SLOTS, *PAGE)
    dma = pltpu.SemaphoreType.DMA
    i32 = jnp.int32
    columns = out_weight.shape[1]
    seqs = NDP * SEQ_DEV
    send, tags, meta = pl.pallas_call(
        pack_kernel,
        name="pack",
        out_shape=[pltpu.VMEM((NDP * CAP, *PAGE), bf16), pltpu.VMEM((NDP, 1, 128), i32), pltpu.VMEM((1, 1, 128), i32)],
        in_specs=[sspec(), sspec(), sspec(), sspec(), hspec()],
        out_specs=[vspec()] * 3,
        scratch_shapes=[pltpu.SMEM((NDP,), i32), dma((MOVES,))],
        compiler_params=pltpu.CompilerParams(vmem_limit_bytes=VMEM_LIMIT),
    )(jnp.transpose(move_plan, (1, 0, 2)), move_count, block_table, seq_lens, kv)
    local, recv, code, projected = pl.pallas_call(
        step_kernel,
        name="step",
        out_shape=[
            pltpu.VMEM((SLOTS, *PAGE), bf16),
            pltpu.VMEM((NDP * CAP, *PAGE), bf16),
            pltpu.VMEM((1, 128), i32),
            pltpu.VMEM((seqs, columns), bf16),
        ],
        in_specs=[sspec(), sspec(), vspec(), vspec(), vspec(), vspec(), vspec(), hspec()],
        out_specs=[vspec()] * 4,
        scratch_shapes=[
            pltpu.VMEM((NDP, 1, 128), i32),
            pltpu.VMEM((NDP, 1, 128), i32),
            pltpu.VMEM((NDP, SEQ_DEV * HEADS, HD), bf16),
            pltpu.VMEM((CAP, NDP, 1, 128), f32),
            pltpu.VMEM((CAP, NDP, 1, 128), f32),
            pltpu.VMEM((CAP, NDP, 1, 128), f32),
            pltpu.VMEM((NDP, CAP, HEADS, HD), bf16),
            pltpu.VMEM((NDP, 1, 128), f32),
            pltpu.VMEM((NDP, CAP, HEADS, HD), bf16),
            pltpu.VMEM((NDP, 1, 128), f32),
            pltpu.VMEM((SEQ_DEV + NDP * CAP, HEADS, 128), f32),
            pltpu.VMEM((SEQ_DEV * HEADS, HD), f32),
            pltpu.VMEM((SEQ_DEV, HEADS * HD), bf16),
            pltpu.VMEM((NDP, SEQ_DEV, HEADS * HD), bf16),
            pltpu.VMEM((seqs, columns), f32),
            pltpu.VMEM((NT, seqs // NT, columns), f32),
            dma(()), dma((WINDOW,)), dma((1,)), dma((2,)), dma((2,)), dma((2,)), dma((2,)),
            dma((NZ,)), dma((NZ,)), dma((NDP,)), dma((NDP,)),
            dma((NZ,)), dma((NZ,)), dma((NDP,)), dma((NDP,)),
            dma((NT,)), dma((NT,)), dma((NT,)), dma((NT,)),
        ],
        compiler_params=pltpu.CompilerParams(
            collective_id=0, has_side_effects=True, vmem_limit_bytes=VMEM_LIMIT
        ),
    )(block_table, seq_lens, send, tags, meta, query.reshape(SEQ_DEV * HEADS, HD), out_weight, kv)
    new_pages, projected = pl.pallas_call(
        place_kernel,
        name="place",
        out_shape=[
            jax.ShapeDtypeStruct((SLOTS, *PAGE), bf16),
            jax.ShapeDtypeStruct((seqs, columns), bf16),
        ],
        in_specs=[sspec(), vspec(), vspec(), vspec()],
        out_specs=[hspec(), hspec()],
        scratch_shapes=[dma((SLOTS,)), dma(())],
        compiler_params=pltpu.CompilerParams(vmem_limit_bytes=VMEM_LIMIT),
    )(code, local, recv, projected)
    return new_pages.reshape(kv_pages.shape), projected


def solution(mesh):
    placed = (
        P("dp", "tensor", None),
        P("dp", "tensor", None, None, None),
        P("dp", None, None),
        P("dp"),
        P("dp", None),
        P("dp"),
        P("tensor", "dp"),
    )
    return jax.shard_map(
        body,
        mesh=mesh,
        in_specs=placed,
        out_specs=(P("dp", "tensor", None, None, None), P(None, "dp")),
        check_vma=False,
    )
```

```python
import functools
import math

import jax
import jax.numpy as jnp
from jax import lax
from jax.experimental import pallas as pl
from jax.experimental.pallas import tpu as pltpu
from jax.sharding import PartitionSpec as P

HD = 128
BLOCK = 128
BLOCKS = 8
CAP = 2
SLOTS = 88
MOVES = 48
NY, NZ = 4, 8
NDP = NY * NZ
NT = 8
SEQ_DEV = 8
HEADS = 8
WINDOW = 16
NEG = -1e30
SCALE = 1.0 / math.sqrt(HD)
MESH = pl.DeviceIdType.MESH
VMEM_LIMIT = 24 * 1024 * 1024
PAGE = (2, BLOCK, HD)
SHIFTS = [(dy, dz) for dy in range(NY) for dz in range(NZ)]
f32 = jnp.float32
bf16 = jnp.bfloat16


def far(shift):
    return min(shift[0], NY - shift[0]) + min(shift[1], NZ - shift[1])


def vspec():
    return pl.BlockSpec(memory_space=pltpu.VMEM)


def sspec():
    return pl.BlockSpec(memory_space=pltpu.SMEM)


def hspec():
    return pl.BlockSpec(memory_space=pltpu.HBM)


def step_kernel(
    count_ref, plan_hbm, table_hbm, lens_hbm, query_hbm, w_hbm, kv_ref,
    comb_ref, code_ref, out_ref,
    plan_ref, table_ref, lens_ref, query_ref, w_ref, local_ref, send_ref, tags_ref, meta_ref, got, metas, qall, src_seq, src_end, arr_seq, part, lse, apart, alse, wide, mixed, att, gath, proj, red,
    in_sems, load_sem, page_send, page_recv, tag_sem, meta_sem, part_sem, lse_sem,
    qz_send, qz_recv, qy_send, qy_recv, z_send, z_recv, y_send, y_recv, r_send, r_recv, o_send, o_recv,
):
    me = lax.axis_index("dp")
    t = lax.axis_index("tensor")
    y, z = me // NZ, me % NZ
    zs = [lax.rem(z + d, NZ) for d in range(NZ)]
    ys = [lax.rem(y + d, NY) for d in range(NY)]
    ts = [lax.rem(t + d, NT) for d in range(NT)]
    fetch = [
        pltpu.make_async_copy(a, b, in_sems.at[i])
        for i, (a, b) in enumerate(
            [(plan_hbm, plan_ref), (query_hbm, query_ref), (table_hbm, table_ref), (lens_hbm, lens_ref), (w_hbm, w_ref)]
        )
    ]
    load = pltpu.make_async_copy(kv_ref, local_ref, load_sem.at[0])
    keep = pltpu.make_async_copy(kv_ref, comb_ref.at[pl.ds(0, SLOTS)], load_sem.at[1])
    for copy in fetch + [load, keep]:
        copy.start()
    bar = pltpu.get_barrier_semaphore()
    order = sorted([s for s in SHIFTS if s != (0, 0)], key=lambda s: -far(s))
    peers = [(ys[dy] * NZ + zs[dz], t) for dy, dz in order] + [(me, ts[d]) for d in range(1, NT)]
    for peer in peers:
        pl.semaphore_signal(bar, inc=1, device_id=peer, device_id_type=MESH)

    i32 = jnp.int32
    for copy in fetch[:4]:
        copy.wait()

    def iota(shape, axis):
        return lax.broadcasted_iota(i32, shape, axis)

    plan = [jnp.broadcast_to(plan_ref[r], (MOVES, MOVES)) for r in range(3)]
    down, across = iota((MOVES, MOVES), 0), iota((MOVES, MOVES), 1)
    target = jnp.sum(jnp.where(down == across, plan[1], 0), axis=1, keepdims=True)
    before = (target == plan[1]) & (down < across) & (down < count_ref[0])
    rank = jnp.sum(jnp.where(before, 1, 0), axis=0, keepdims=True)
    goes = plan_ref[1]
    shift = (((goes >> 3) - y) & (NY - 1)) * NZ + ((goes - z) & (NZ - 1))
    row = jnp.where(iota((1, MOVES), 1) < count_ref[0], shift * CAP + rank, -1)
    lane = iota((NDP, 128), 1)
    tags = jnp.full((NDP, 128), -1, i32)
    source = []
    for c in range(CAP):
        hit = jnp.broadcast_to(row, (NDP, MOVES)) == iota((NDP, MOVES), 0) * CAP + c
        source.append(
            jnp.sum(jnp.where(hit, jnp.broadcast_to(plan_ref[0], (NDP, MOVES)), 0), axis=1, keepdims=True)
        )
        slot = jnp.sum(jnp.where(hit, jnp.broadcast_to(plan_ref[2], (NDP, MOVES)) + 1, 0), axis=1, keepdims=True) - 1
        tags = jnp.where(lane == c, slot, tags)
    tags_ref[...] = tags.reshape(NDP, 1, 128)
    lane1 = iota((1, 128), 1)
    meta = jnp.full((1, 128), -2, i32)
    for s in range(SEQ_DEV):
        for b in range(BLOCKS):
            meta = jnp.where(lane1 == s * BLOCKS + b, table_ref[s, b], meta)
        meta = jnp.where(lane1 == SEQ_DEV * BLOCKS + s, lens_ref[s], meta)
    meta_ref[0] = meta
    load.wait()

    def take(c, k):
        send_ref[k * CAP + c] = local_ref[source[c][k, 0]]

    for c, (dy, dz) in [(c, s) for c in range(CAP) for s in order]:
        take(c, dy * NZ + dz)
    for c in range(CAP):
        take(c, 0)
    pl.semaphore_wait(bar, len(peers))

    def remote(src, dst, send, recv, device):
        copy = pltpu.make_async_remote_copy(
            src_ref=src, dst_ref=dst, send_sem=send, recv_sem=recv, device_id=device, device_id_type=MESH
        )
        copy.start()
        return copy

    def to(shift):
        return (ys[shift[0]] * NZ + zs[shift[1]], t)

    def at(shift):
        return shift[0] * NZ + shift[1]

    pages = []
    pending = [(c, s) for c in range(CAP) for s in order]

    def pump(n):
        for _ in range(n):
            i = len(pages)
            if i >= len(pending):
                return
            if i >= WINDOW:
                pages[i - WINDOW].wait_send()
            c, s = pending[i]
            row = at(s) * CAP + c
            pages.append(
                remote(send_ref.at[row], comb_ref.at[SLOTS + row], page_send.at[i % WINDOW], page_recv.at[0], to(s))
            )

    z_order = sorted(range(1, NZ), key=lambda d: -min(d, NZ - d))
    z_near = sorted(range(1, NZ), key=lambda d: min(d, NZ - d))

    def gather_start(own_ref, buf, zsend, zrecv, ysend, yrecv):
        along_z = {d: remote(own_ref, buf.at[me], zsend.at[d], zrecv.at[d], (y * NZ + zs[d], t)) for d in z_order}
        along_y = [
            remote(own_ref, buf.at[me], ysend.at[d], yrecv.at[d], (ys[d] * NZ + z, t)) for d in (2, 1, 3)
        ]
        buf[me] = own_ref[...]
        return along_z, along_y

    def gather_forward(along_z, along_y, buf, ysend, yrecv, pumps):
        for e in z_near:
            along_z[e].wait_recv()
            held = y * NZ + lax.rem(z - e + NZ, NZ)
            for d in (2, 1, 3):
                n = e * NY + d
                along_y.append(
                    remote(buf.at[held], buf.at[held], ysend.at[n], yrecv.at[n], (ys[d] * NZ + z, t))
                )
            pump(pumps)

    q_z, q_y = gather_start(query_ref, qall, qz_send, qz_recv, qy_send, qy_recv)
    small = []
    for s in order:
        back = ((NY - s[0]) % NY, (NZ - s[1]) % NZ)
        small.append(remote(tags_ref.at[at(s)], got.at[at(s)], tag_sem.at[0], tag_sem.at[1], to(s)))
        small.append(remote(meta_ref.at[0], metas.at[at(back)], meta_sem.at[0], meta_sem.at[1], to(s)))
    got[0] = tags_ref[0]
    metas[0] = meta_ref[0]
    pump(WINDOW)
    comb_ref[SLOTS : SLOTS + CAP] = send_ref[0:CAP]
    gather_forward(q_z, q_y, qall, qy_send, qy_recv, 1)

    def all_of(buf, sems):
        return pltpu.make_async_remote_copy(
            src_ref=buf.at[pl.ds(1, NDP - 1)],
            dst_ref=buf.at[pl.ds(1, NDP - 1)],
            send_sem=sems.at[0],
            recv_sem=sems.at[1],
            device_id=(me, ts[1]),
            device_id_type=MESH,
        )

    all_of(got, tag_sem).wait_recv()
    all_of(metas, meta_sem).wait_recv()
    lane_f = lane.astype(f32)
    first = lane < SEQ_DEV * BLOCKS
    seq_f = (lane // BLOCKS).astype(f32)
    block_f = (lane % BLOCKS).astype(f32)
    device_f = lax.broadcasted_iota(jnp.int32, (NDP, 128), 0).astype(f32)
    mine = metas[0]
    moved = jnp.zeros((1, 128), f32)
    code = lane1.astype(f32)
    sent_tags = tags_ref[...].reshape(NDP, 128)
    got_tags = got[...].reshape(NDP, 128)
    tables = metas[...].reshape(NDP, 128)

    def spread(column):
        return jnp.broadcast_to(column, (NDP, 128)).reshape(NDP, 1, 128)

    for c in range(CAP):
        tag = sent_tags[:, c : c + 1]
        hit = (tables == tag) & first & (tag >= 0)
        found = jnp.sum(jnp.where(hit, 1.0, 0.0), axis=1, keepdims=True)
        seq = jnp.sum(jnp.where(hit, seq_f, 0.0), axis=1, keepdims=True)
        block = jnp.sum(jnp.where(hit, block_f, 0.0), axis=1, keepdims=True)
        ends = jnp.sum(
            jnp.where(lane_f == seq + SEQ_DEV * BLOCKS, tables.astype(f32), 0.0), axis=1, keepdims=True
        )
        src_seq[c] = spread(jnp.where(found > 0, seq, -1.0))
        src_end[c] = spread(ends - block * BLOCK)
        tag = got_tags[:, c : c + 1]
        hit = (mine == tag) & first & (tag >= 0)
        found = jnp.sum(jnp.where(hit, 1.0, 0.0), axis=1, keepdims=True)
        seq = jnp.sum(jnp.where(hit, seq_f, 0.0), axis=1, keepdims=True)
        arr_seq[c] = spread(jnp.where(found > 0, seq, -1.0))
        moved = jnp.maximum(moved, jnp.max(jnp.where(hit, 1.0, 0.0), axis=0, keepdims=True))
        code = code + jnp.sum(
            jnp.where(lane == tag, device_f * CAP + (SLOTS + c) - lane_f, 0.0), axis=0, keepdims=True
        )
    code_ref[...] = code.astype(jnp.int32)
    pump(2)

    keep.wait()
    position = lax.broadcasted_iota(jnp.int32, (HEADS, BLOCKS * BLOCK), 1)
    kept_o = []
    kept_lse = []
    for s in range(SEQ_DEV):
        index = [table_ref[s, b] for b in range(BLOCKS)]
        keys = jnp.concatenate([local_ref[i, 0] for i in index], axis=0)
        scores = lax.dot_general(
            query_ref[s * HEADS : (s + 1) * HEADS, :], keys, (((1,), (1,)), ((), ())), preferred_element_type=f32
        ) * SCALE
        gone = jnp.concatenate(
            [jnp.broadcast_to(moved[:, s * BLOCKS + b : s * BLOCKS + b + 1], (1, BLOCK)) for b in range(BLOCKS)], axis=1
        )
        scores = jnp.where((position < lens_ref[s]) & (gone == 0), scores, NEG)
        largest = jnp.max(scores, axis=1, keepdims=True)
        expo = jnp.exp(scores - largest)
        total = jnp.sum(expo, axis=1, keepdims=True)
        values = jnp.concatenate([local_ref[i, 1] for i in index], axis=0)
        mixed[s * HEADS : (s + 1) * HEADS, :] = (
            jnp.dot(expo.astype(bf16), values, preferred_element_type=f32) / total
        )
        wide[s] = jnp.broadcast_to(largest + jnp.log(total), (HEADS, 128))
        if s % 2:
            pump(1)

    for copy in q_y:
        copy.wait_recv()
    lane8 = lax.broadcasted_iota(jnp.int32, (HEADS, 128), 1)
    row8 = lax.broadcasted_iota(jnp.int32, (HEADS, 128), 0)
    lane8_f = lane8.astype(f32)

    def rows8(ref, c, k):
        return jnp.broadcast_to(ref[c, k], (HEADS, 128))

    def partial(k, carry):
        dy, dz = k // NZ, lax.rem(k, NZ)
        owner = lax.rem(y + dy, NY) * NZ + lax.rem(z + dz, NZ)
        asked = qall[owner]
        keys = jnp.concatenate([send_ref[k * CAP + c, 0] for c in range(CAP)], axis=0)
        every = lax.dot_general(asked, keys, (((1,), (1,)), ((), ())), preferred_element_type=f32) * SCALE
        row = jnp.zeros((1, 128), f32)
        for c in range(CAP):
            seq = rows8(src_seq, c, k)
            scores = jnp.full((HEADS, BLOCK), NEG, f32)
            for s in range(SEQ_DEV):
                scores = jnp.where(
                    seq == s, every[s * HEADS : (s + 1) * HEADS, c * BLOCK : (c + 1) * BLOCK], scores
                )
            scores = jnp.where(lane8_f < rows8(src_end, c, k), scores, NEG)
            largest = jnp.max(scores, axis=1, keepdims=True)
            expo = jnp.exp(scores - largest)
            total = jnp.sum(expo, axis=1, keepdims=True)
            o = jnp.dot(expo.astype(bf16), send_ref[k * CAP + c, 1], preferred_element_type=f32) / total
            part[k, c] = jnp.where(seq >= 0, o, 0.0).astype(bf16)
            weight = jnp.where(seq >= 0, largest + jnp.log(total), NEG)
            row = row + jnp.sum(jnp.where(lane8 == row8 + c * HEADS, weight, 0.0), axis=0, keepdims=True)
        lse[k] = row
        return carry

    for g in range(4):
        lax.fori_loop(g * NZ, (g + 1) * NZ, partial, 0)
        for dz in range(NZ):
            if (g, dz) != (0, 0):
                k = at((g, dz))
                small.append(remote(part.at[k], apart.at[k], part_sem.at[0], part_sem.at[1], to((g, dz))))
                small.append(remote(lse.at[k], alse.at[k], lse_sem.at[0], lse_sem.at[1], to((g, dz))))
        pump(2)
    apart[0] = part[0]
    alse[0] = lse[0]
    pump(3)
    all_of(apart, part_sem).wait_recv()
    all_of(alse, lse_sem).wait_recv()

    def widen(k, tops):
        tops = list(tops)
        for c in range(CAP):
            column = jnp.sum(
                jnp.where(lane8 == row8 + c * HEADS, jnp.broadcast_to(alse[k], (HEADS, 128)), 0.0),
                axis=1,
                keepdims=True,
            )
            full = jnp.broadcast_to(column, (HEADS, 128))
            wide[SEQ_DEV + k * CAP + c] = full
            seq = rows8(arr_seq, c, k)
            for s in range(SEQ_DEV):
                tops[s] = jnp.where(seq == s, jnp.maximum(tops[s], full), tops[s])
        return tuple(tops)

    tops = lax.fori_loop(0, NDP, widen, tuple(wide[s] for s in range(SEQ_DEV)))
    start = []
    for s in range(SEQ_DEV):
        w = jnp.exp(wide[s] - tops[s])
        start.append((w, w * mixed[s * HEADS : (s + 1) * HEADS, :]))

    def merge(k, sums):
        dens, nums = list(sums[0]), list(sums[1])
        for c in range(CAP):
            seq = rows8(arr_seq, c, k)
            top = jnp.zeros((HEADS, 128), f32)
            for s in range(SEQ_DEV):
                top = jnp.where(seq == s, tops[s], top)
            w = jnp.exp(wide[SEQ_DEV + k * CAP + c] - top)
            o = w * apart[k, c].astype(f32)
            for s in range(SEQ_DEV):
                dens[s] = jnp.where(seq == s, dens[s] + w, dens[s])
                nums[s] = jnp.where(seq == s, nums[s] + o, nums[s])
        return tuple(dens), tuple(nums)

    dens, nums = lax.fori_loop(
        0, NDP, merge, (tuple(a for a, _ in start), tuple(b for _, b in start))
    )
    for s in range(SEQ_DEV):
        mixed[s * HEADS : (s + 1) * HEADS, :] = nums[s] / dens[s]
    att[...] = jnp.concatenate(
        [mixed[pl.ds(h, SEQ_DEV, stride=HEADS), :] for h in range(HEADS)], axis=1
    ).astype(bf16)

    along_z, along_y = gather_start(att, gath, z_send, z_recv, y_send, y_recv)
    pump(4)
    gather_forward(along_z, along_y, gath, y_send, y_recv, 1)
    pump(2)
    for copy in along_y:
        copy.wait_recv()
    fetch[4].wait()
    rows = gath[...].reshape(NDP * SEQ_DEV, HEADS * HD)
    proj[...] = jnp.dot(rows, w_ref[...], preferred_element_type=f32)
    chunk = NDP * SEQ_DEV // NT
    t_order = (4, 5, 3, 2, 6, 1, 7)

    def rows_of(i):
        return pl.ds(pl.multiple_of(i * chunk, chunk), chunk)

    sums = [remote(proj.at[rows_of(ts[d])], red.at[d], r_send.at[d], r_recv.at[d], (me, ts[d])) for d in t_order]
    pump(2)
    total = proj[rows_of(t), :]
    for copy in sums:
        copy.wait_recv()
    for d in range(1, NT):
        total = total + red[d]
    out_ref[rows_of(t), :] = total.astype(bf16)
    outs = [
        remote(out_ref.at[rows_of(t)], out_ref.at[rows_of(t)], o_send.at[d], o_recv.at[d], (me, ts[d])) for d in t_order
    ]
    pump(len(pending))
    for copy in outs:
        copy.wait_recv()
    for copy in pages[-WINDOW:]:
        copy.wait_send()
    for copy in list(q_z.values()) + q_y + list(along_z.values()) + along_y + sums + outs:
        copy.wait_send()
    all_of(got, tag_sem).wait_send()
    all_of(metas, meta_sem).wait_send()
    all_of(part, part_sem).wait_send()
    all_of(lse, lse_sem).wait_send()
    moved_pages = comb_ref.at[pl.ds(SLOTS + CAP, (NDP - 1) * CAP)]
    pltpu.make_async_remote_copy(
        src_ref=moved_pages, dst_ref=moved_pages, send_sem=page_send.at[0], recv_sem=page_recv.at[0],
        device_id=(me, ts[1]), device_id_type=MESH,
    ).wait_recv()


def place_kernel(code_ref, comb_ref, proj_ref, new_ref, out_ref, sems, out_sem):
    copies = []
    for s in range(SLOTS):
        copies.append(pltpu.make_async_copy(comb_ref.at[code_ref[0, s]], new_ref.at[s], sems.at[s]))
        copies[-1].start()
    copies.append(pltpu.make_async_copy(proj_ref, out_ref, out_sem))
    copies[-1].start()
    for copy in copies:
        copy.wait()


def body(query, kv_pages, move_plan, move_count, block_table, seq_lens, out_weight):
    def in_hbm(x):
        return pltpu.with_memory_space_constraint(x, pltpu.HBM)

    kv = in_hbm(kv_pages.reshape(SLOTS, *PAGE))
    table = in_hbm(block_table)
    lens = in_hbm(seq_lens)
    dma = pltpu.SemaphoreType.DMA
    i32 = jnp.int32
    columns = out_weight.shape[1]
    seqs = NDP * SEQ_DEV
    comb, code, projected = pl.pallas_call(
        step_kernel,
        name="step",
        out_shape=[
            pltpu.VMEM((SLOTS + NDP * CAP, *PAGE), bf16),
            pltpu.VMEM((1, 128), i32),
            pltpu.VMEM((seqs, columns), bf16),
        ],
        in_specs=[sspec()] + [hspec()] * 6,
        out_specs=[vspec()] * 3,
        scratch_shapes=[
            pltpu.VMEM((3, 1, MOVES), i32),
            pltpu.SMEM((SEQ_DEV, BLOCKS), i32),
            pltpu.SMEM((SEQ_DEV,), i32),
            pltpu.VMEM((SEQ_DEV * HEADS, HD), bf16),
            pltpu.VMEM(out_weight.shape, bf16),
            pltpu.VMEM((SLOTS, *PAGE), bf16),
            pltpu.VMEM((NDP * CAP, *PAGE), bf16),
            pltpu.VMEM((NDP, 1, 128), i32),
            pltpu.VMEM((1, 1, 128), i32),
            pltpu.VMEM((NDP, 1, 128), i32),
            pltpu.VMEM((NDP, 1, 128), i32),
            pltpu.VMEM((NDP, SEQ_DEV * HEADS, HD), bf16),
            pltpu.VMEM((CAP, NDP, 1, 128), f32),
            pltpu.VMEM((CAP, NDP, 1, 128), f32),
            pltpu.VMEM((CAP, NDP, 1, 128), f32),
            pltpu.VMEM((NDP, CAP, HEADS, HD), bf16),
            pltpu.VMEM((NDP, 1, 128), f32),
            pltpu.VMEM((NDP, CAP, HEADS, HD), bf16),
            pltpu.VMEM((NDP, 1, 128), f32),
            pltpu.VMEM((SEQ_DEV + NDP * CAP, HEADS, 128), f32),
            pltpu.VMEM((SEQ_DEV * HEADS, HD), f32),
            pltpu.VMEM((SEQ_DEV, HEADS * HD), bf16),
            pltpu.VMEM((NDP, SEQ_DEV, HEADS * HD), bf16),
            pltpu.VMEM((seqs, columns), f32),
            pltpu.VMEM((NT, seqs // NT, columns), f32),
            dma((5,)), dma((2,)), dma((WINDOW,)), dma((1,)), dma((2,)), dma((2,)), dma((2,)), dma((2,)),
            dma((NZ,)), dma((NZ,)), dma((NDP,)), dma((NDP,)),
            dma((NZ,)), dma((NZ,)), dma((NDP,)), dma((NDP,)),
            dma((NT,)), dma((NT,)), dma((NT,)), dma((NT,)),
        ],
        compiler_params=pltpu.CompilerParams(
            collective_id=0, has_side_effects=True, vmem_limit_bytes=VMEM_LIMIT
        ),
    )(move_count, in_hbm(jnp.transpose(move_plan, (1, 0, 2))), table, lens, in_hbm(query.reshape(SEQ_DEV * HEADS, HD)), in_hbm(out_weight), kv)
    new_pages, projected = pl.pallas_call(
        place_kernel,
        name="place",
        out_shape=[
            jax.ShapeDtypeStruct((SLOTS, *PAGE), bf16),
            jax.ShapeDtypeStruct((seqs, columns), bf16),
        ],
        in_specs=[sspec(), vspec(), vspec()],
        out_specs=[hspec(), hspec()],
        scratch_shapes=[dma((SLOTS,)), dma(())],
        compiler_params=pltpu.CompilerParams(vmem_limit_bytes=VMEM_LIMIT),
    )(code, comb, projected)
    return new_pages.reshape(kv_pages.shape), projected


def solution(mesh):
    placed = (
        P("dp", "tensor", None),
        P("dp", "tensor", None, None, None),
        P("dp", None, None),
        P("dp"),
        P("dp", None),
        P("dp"),
        P("tensor", "dp"),
    )
    return jax.shard_map(
        body,
        mesh=mesh,
        in_specs=placed,
        out_specs=(P("dp", "tensor", None, None, None), P(None, "dp")),
        check_vma=False,
    )
```

```python
import functools
import math

import jax
import jax.numpy as jnp
from jax import lax
from jax.experimental import pallas as pl
from jax.experimental.pallas import tpu as pltpu
from jax.sharding import PartitionSpec as P

HD = 128
BLOCK = 128
BLOCKS = 8
CAP = 2
SLOTS = 88
MOVES = 48
NY, NZ = 4, 8
NDP = NY * NZ
NT = 8
SEQ_DEV = 8
HEADS = 8
WINDOW = 12
TAG_LANE = SEQ_DEV * BLOCKS + SEQ_DEV
NEG = -1e30
SCALE = 1.0 / math.sqrt(HD)
MESH = pl.DeviceIdType.MESH
VMEM_LIMIT = 24 * 1024 * 1024
PAGE = (2, BLOCK, HD)
SHIFTS = [(dy, dz) for dy in range(NY) for dz in range(NZ)]
f32 = jnp.float32
bf16 = jnp.bfloat16


def far(shift):
    return min(shift[0], NY - shift[0]) + min(shift[1], NZ - shift[1])


def vspec():
    return pl.BlockSpec(memory_space=pltpu.VMEM)


def sspec():
    return pl.BlockSpec(memory_space=pltpu.SMEM)


def hspec():
    return pl.BlockSpec(memory_space=pltpu.HBM)


def step_kernel(
    count_ref, plan_hbm, table_hbm, lens_hbm, query_hbm, w_hbm, kv_ref,
    comb_ref, code_ref, out_ref,
    plan_ref, table_ref, lens_ref, query_ref, w_ref, local_ref, send_ref, tags_ref,
    got, qall, src_seq, src_end, arr_seq, part, lse, apart, alse, wide, mixed, att, gath, proj, red,
    in_sems, load_sem, page_send, page_recv, tag_sem, part_sem, lse_sem,
    qz_send, qz_recv, qy_send, qy_recv, z_send, z_recv, y_send, y_recv, r_send, r_recv, o_send, o_recv,
):
    me = lax.axis_index("dp")
    t = lax.axis_index("tensor")
    y, z = me // NZ, me % NZ
    zs = [lax.rem(z + d, NZ) for d in range(NZ)]
    ys = [lax.rem(y + d, NY) for d in range(NY)]
    ts = [lax.rem(t + d, NT) for d in range(NT)]
    bar = pltpu.get_barrier_semaphore()
    order = sorted([s for s in SHIFTS if s != (0, 0)], key=lambda s: -far(s))
    peers = [(ys[dy] * NZ + zs[dz], t) for dy, dz in order] + [(me, ts[d]) for d in range(1, NT)]
    for peer in peers:
        pl.semaphore_signal(bar, inc=1, device_id=peer, device_id_type=MESH)
    fetch = [
        pltpu.make_async_copy(a, b, in_sems.at[i])
        for i, (a, b) in enumerate(
            [(plan_hbm, plan_ref), (query_hbm, query_ref), (table_hbm, table_ref), (lens_hbm, lens_ref), (w_hbm, w_ref)]
        )
    ]
    load = pltpu.make_async_copy(kv_ref, local_ref, load_sem.at[0])
    keep = pltpu.make_async_copy(kv_ref, comb_ref.at[pl.ds(0, SLOTS)], load_sem.at[1])
    for copy in fetch[:4] + [load]:
        copy.start()

    i32 = jnp.int32
    for copy in fetch[:4]:
        copy.wait()

    def iota(shape, axis):
        return lax.broadcasted_iota(i32, shape, axis)

    plan = [jnp.broadcast_to(plan_ref[r], (MOVES, MOVES)) for r in range(3)]
    down, across = iota((MOVES, MOVES), 0), iota((MOVES, MOVES), 1)
    target = jnp.sum(jnp.where(down == across, plan[1], 0), axis=1, keepdims=True)
    before = (target == plan[1]) & (down < across) & (down < count_ref[0])
    rank = jnp.sum(jnp.where(before, 1, 0), axis=0, keepdims=True)
    goes = plan_ref[1]
    shift = (((goes >> 3) - y) & (NY - 1)) * NZ + ((goes - z) & (NZ - 1))
    row = jnp.where(iota((1, MOVES), 1) < count_ref[0], shift * CAP + rank, -1)
    lane = iota((NDP, 128), 1)
    lane1 = iota((1, 128), 1)
    meta = jnp.full((1, 128), -2, i32)
    for s in range(SEQ_DEV):
        for b in range(BLOCKS):
            meta = jnp.where(lane1 == s * BLOCKS + b, table_ref[s, b], meta)
        meta = jnp.where(lane1 == SEQ_DEV * BLOCKS + s, lens_ref[s], meta)
    tags = jnp.broadcast_to(meta, (NDP, 128))
    source = []
    for c in range(CAP):
        hit = jnp.broadcast_to(row, (NDP, MOVES)) == iota((NDP, MOVES), 0) * CAP + c
        source.append(
            jnp.sum(jnp.where(hit, jnp.broadcast_to(plan_ref[0], (NDP, MOVES)), 0), axis=1, keepdims=True)
        )
        slot = jnp.sum(jnp.where(hit, jnp.broadcast_to(plan_ref[2], (NDP, MOVES)) + 1, 0), axis=1, keepdims=True) - 1
        tags = jnp.where(lane == TAG_LANE + c, slot, tags)
    tags_ref[...] = tags.reshape(NDP, 1, 128)
    load.wait()
    keep.start()
    fetch[4].start()

    def take(c, k):
        send_ref[k * CAP + c] = local_ref[source[c][k, 0]]

    for c, (dy, dz) in [(c, s) for c in range(CAP) for s in order]:
        take(c, dy * NZ + dz)
    for c in range(CAP):
        take(c, 0)
    pl.semaphore_wait(bar, len(peers))

    def remote(src, dst, send, recv, device):
        copy = pltpu.make_async_remote_copy(
            src_ref=src, dst_ref=dst, send_sem=send, recv_sem=recv, device_id=device, device_id_type=MESH
        )
        copy.start()
        return copy

    def to(shift):
        return (ys[shift[0]] * NZ + zs[shift[1]], t)

    def at(shift):
        return shift[0] * NZ + shift[1]

    pages = []
    pending = [(c, s) for c in range(CAP) for s in order]

    def pump(n):
        for _ in range(n):
            i = len(pages)
            if i >= len(pending):
                return
            if i >= WINDOW:
                pages[i - WINDOW].wait_send()
            c, s = pending[i]
            row = at(s) * CAP + c
            pages.append(
                remote(send_ref.at[row], comb_ref.at[SLOTS + row], page_send.at[i % WINDOW], page_recv.at[0], to(s))
            )

    relays = {2: (1, 2), 6: (7,)}

    def gather_start(own_ref, buf, zsend, zrecv, ysend, yrecv, sign):
        along_z = {}
        for d in (2, 6, 1, 7):
            e = d * sign % NZ
            along_z[e] = remote(own_ref, buf.at[me], zsend.at[e], zrecv.at[e], (y * NZ + zs[e], t))
        along_y = [
            remote(own_ref, buf.at[me], ysend.at[d], yrecv.at[d], (ys[d] * NZ + z, t)) for d in (2, 1, 3)
        ]
        buf[me] = own_ref[...]
        return along_z, along_y

    def gather_forward(along_z, along_y, buf, zsend, zrecv, ysend, yrecv, sign, pumps):
        for d in (2, 6, 1, 7, 3, 5, 4):
            e = d * sign % NZ
            along_z[e].wait_recv()
            held = y * NZ + lax.rem(z - e + NZ, NZ)
            for step in relays.get(d, ()):
                there = (d + step) * sign % NZ
                along_z[there] = remote(
                    buf.at[held], buf.at[held], zsend.at[there], zrecv.at[there],
                    (y * NZ + zs[step * sign % NZ], t),
                )
            for d_y in (2, 1, 3):
                n = e * NY + d_y
                along_y.append(
                    remote(buf.at[held], buf.at[held], ysend.at[n], yrecv.at[n], (ys[d_y] * NZ + z, t))
                )
            pump(pumps)

    q_z, q_y = gather_start(query_ref, qall, qz_send, qz_recv, qy_send, qy_recv, 1)
    small = []
    for s in order:
        small.append(remote(tags_ref.at[at(s)], got.at[at(s)], tag_sem.at[0], tag_sem.at[1], to(s)))
    got[0] = tags_ref[0]
    pump(WINDOW)
    comb_ref[SLOTS : SLOTS + CAP] = send_ref[0:CAP]
    gather_forward(q_z, q_y, qall, qz_send, qz_recv, qy_send, qy_recv, 1, 1)

    def all_of(buf, sems):
        return pltpu.make_async_remote_copy(
            src_ref=buf.at[pl.ds(1, NDP - 1)],
            dst_ref=buf.at[pl.ds(1, NDP - 1)],
            send_sem=sems.at[0],
            recv_sem=sems.at[1],
            device_id=(me, ts[1]),
            device_id_type=MESH,
        )

    all_of(got, tag_sem).wait_recv()
    lane_f = lane.astype(f32)
    first = lane < SEQ_DEV * BLOCKS
    seq_f = (lane // BLOCKS).astype(f32)
    block_f = (lane % BLOCKS).astype(f32)
    device_f = lax.broadcasted_iota(jnp.int32, (NDP, 128), 0).astype(f32)
    mine = got[0]
    moved = jnp.zeros((1, 128), f32)
    code = lane1.astype(f32)
    sent_tags = tags_ref[...].reshape(NDP, 128)
    got_tags = got[...].reshape(NDP, 128)
    tables = jnp.concatenate([got[at(((NY - dy) % NY, (NZ - dz) % NZ))] for dy, dz in SHIFTS], axis=0)

    def spread(column):
        return jnp.broadcast_to(column, (NDP, 128)).reshape(NDP, 1, 128)

    for c in range(CAP):
        tag = sent_tags[:, TAG_LANE + c : TAG_LANE + c + 1]
        hit = (tables == tag) & first & (tag >= 0)
        found = jnp.sum(jnp.where(hit, 1.0, 0.0), axis=1, keepdims=True)
        seq = jnp.sum(jnp.where(hit, seq_f, 0.0), axis=1, keepdims=True)
        block = jnp.sum(jnp.where(hit, block_f, 0.0), axis=1, keepdims=True)
        ends = jnp.sum(
            jnp.where(lane_f == seq + SEQ_DEV * BLOCKS, tables.astype(f32), 0.0), axis=1, keepdims=True
        )
        src_seq[c] = spread(jnp.where(found > 0, seq, -1.0))
        src_end[c] = spread(ends - block * BLOCK)
        tag = got_tags[:, TAG_LANE + c : TAG_LANE + c + 1]
        hit = (mine == tag) & first & (tag >= 0)
        found = jnp.sum(jnp.where(hit, 1.0, 0.0), axis=1, keepdims=True)
        seq = jnp.sum(jnp.where(hit, seq_f, 0.0), axis=1, keepdims=True)
        arr_seq[c] = spread(jnp.where(found > 0, seq, -1.0))
        moved = jnp.maximum(moved, jnp.max(jnp.where(hit, 1.0, 0.0), axis=0, keepdims=True))
        code = code + jnp.sum(
            jnp.where(lane == tag, device_f * CAP + (SLOTS + c) - lane_f, 0.0), axis=0, keepdims=True
        )
    code_ref[...] = code.astype(jnp.int32)
    pump(2)

    keep.wait()
    position = lax.broadcasted_iota(jnp.int32, (HEADS, BLOCKS * BLOCK), 1)
    kept_o = []
    kept_lse = []
    for s in range(SEQ_DEV):
        index = [table_ref[s, b] for b in range(BLOCKS)]
        keys = jnp.concatenate([local_ref[i, 0] for i in index], axis=0)
        scores = lax.dot_general(
            query_ref[s * HEADS : (s + 1) * HEADS, :], keys, (((1,), (1,)), ((), ())), preferred_element_type=f32
        ) * SCALE
        gone = jnp.concatenate(
            [jnp.broadcast_to(moved[:, s * BLOCKS + b : s * BLOCKS + b + 1], (1, BLOCK)) for b in range(BLOCKS)], axis=1
        )
        scores = jnp.where((position < lens_ref[s]) & (gone == 0), scores, NEG)
        largest = jnp.max(scores, axis=1, keepdims=True)
        expo = jnp.exp(scores - largest)
        total = jnp.sum(expo, axis=1, keepdims=True)
        values = jnp.concatenate([local_ref[i, 1] for i in index], axis=0)
        mixed[s * HEADS : (s + 1) * HEADS, :] = (
            jnp.dot(expo.astype(bf16), values, preferred_element_type=f32) / total
        )
        wide[s] = jnp.broadcast_to(largest + jnp.log(total), (HEADS, 128))
        if s % 2:
            pump(1)

    for copy in q_y:
        copy.wait_recv()
    lane8 = lax.broadcasted_iota(jnp.int32, (HEADS, 128), 1)
    row8 = lax.broadcasted_iota(jnp.int32, (HEADS, 128), 0)
    lane8_f = lane8.astype(f32)

    def rows8(ref, c, k):
        return jnp.broadcast_to(ref[c, k], (HEADS, 128))

    def partial(k, carry):
        dy, dz = k // NZ, lax.rem(k, NZ)
        owner = lax.rem(y + dy, NY) * NZ + lax.rem(z + dz, NZ)
        asked = qall[owner]
        keys = jnp.concatenate([send_ref[k * CAP + c, 0] for c in range(CAP)], axis=0)
        every = lax.dot_general(asked, keys, (((1,), (1,)), ((), ())), preferred_element_type=f32) * SCALE
        row = jnp.zeros((1, 128), f32)
        for c in range(CAP):
            seq = rows8(src_seq, c, k)
            scores = jnp.full((HEADS, BLOCK), NEG, f32)
            for s in range(SEQ_DEV):
                scores = jnp.where(
                    seq == s, every[s * HEADS : (s + 1) * HEADS, c * BLOCK : (c + 1) * BLOCK], scores
                )
            scores = jnp.where(lane8_f < rows8(src_end, c, k), scores, NEG)
            largest = jnp.max(scores, axis=1, keepdims=True)
            expo = jnp.exp(scores - largest)
            total = jnp.sum(expo, axis=1, keepdims=True)
            o = jnp.dot(expo.astype(bf16), send_ref[k * CAP + c, 1], preferred_element_type=f32) / total
            part[k, c] = jnp.where(seq >= 0, o, 0.0).astype(bf16)
            weight = jnp.where(seq >= 0, largest + jnp.log(total), NEG)
            row = row + jnp.sum(jnp.where(lane8 == row8 + c * HEADS, weight, 0.0), axis=0, keepdims=True)
        lse[k] = row
        return carry

    for g in range(4):
        lax.fori_loop(g * NZ, (g + 1) * NZ, partial, 0)
        for dz in range(NZ):
            if (g, dz) != (0, 0):
                k = at((g, dz))
                small.append(remote(part.at[k], apart.at[k], part_sem.at[0], part_sem.at[1], to((g, dz))))
                small.append(remote(lse.at[k], alse.at[k], lse_sem.at[0], lse_sem.at[1], to((g, dz))))
        pump(2)
    apart[0] = part[0]
    alse[0] = lse[0]
    pump(3)
    all_of(apart, part_sem).wait_recv()
    all_of(alse, lse_sem).wait_recv()

    def widen(k, tops):
        tops = list(tops)
        for c in range(CAP):
            column = jnp.sum(
                jnp.where(lane8 == row8 + c * HEADS, jnp.broadcast_to(alse[k], (HEADS, 128)), 0.0),
                axis=1,
                keepdims=True,
            )
            full = jnp.broadcast_to(column, (HEADS, 128))
            wide[SEQ_DEV + k * CAP + c] = full
            seq = rows8(arr_seq, c, k)
            for s in range(SEQ_DEV):
                tops[s] = jnp.where(seq == s, jnp.maximum(tops[s], full), tops[s])
        return tuple(tops)

    tops = lax.fori_loop(0, NDP, widen, tuple(wide[s] for s in range(SEQ_DEV)))
    start = []
    for s in range(SEQ_DEV):
        w = jnp.exp(wide[s] - tops[s])
        start.append((w, w * mixed[s * HEADS : (s + 1) * HEADS, :]))

    def merge(k, sums):
        dens, nums = list(sums[0]), list(sums[1])
        for c in range(CAP):
            seq = rows8(arr_seq, c, k)
            top = jnp.zeros((HEADS, 128), f32)
            for s in range(SEQ_DEV):
                top = jnp.where(seq == s, tops[s], top)
            w = jnp.exp(wide[SEQ_DEV + k * CAP + c] - top)
            o = w * apart[k, c].astype(f32)
            for s in range(SEQ_DEV):
                dens[s] = jnp.where(seq == s, dens[s] + w, dens[s])
                nums[s] = jnp.where(seq == s, nums[s] + o, nums[s])
        return tuple(dens), tuple(nums)

    dens, nums = lax.fori_loop(
        0, NDP, merge, (tuple(a for a, _ in start), tuple(b for _, b in start))
    )
    for s in range(SEQ_DEV):
        mixed[s * HEADS : (s + 1) * HEADS, :] = nums[s] / dens[s]
    att[...] = jnp.concatenate(
        [mixed[pl.ds(h, SEQ_DEV, stride=HEADS), :] for h in range(HEADS)], axis=1
    ).astype(bf16)

    along_z, along_y = gather_start(att, gath, z_send, z_recv, y_send, y_recv, -1)
    pump(4)
    gather_forward(along_z, along_y, gath, z_send, z_recv, y_send, y_recv, -1, 1)
    pump(2)
    for copy in along_y:
        copy.wait_recv()
    fetch[4].wait()
    rows = gath[...].reshape(NDP * SEQ_DEV, HEADS * HD)
    proj[...] = jnp.dot(rows, w_ref[...], preferred_element_type=f32)
    chunk = NDP * SEQ_DEV // NT
    t_order = (4, 5, 3, 2, 6, 1, 7)

    def rows_of(i):
        return pl.ds(pl.multiple_of(i * chunk, chunk), chunk)

    sums = [remote(proj.at[rows_of(ts[d])], red.at[d], r_send.at[d], r_recv.at[d], (me, ts[d])) for d in t_order]
    pump(2)
    total = proj[rows_of(t), :]
    for copy in sums:
        copy.wait_recv()
    for d in range(1, NT):
        total = total + red[d]
    out_ref[rows_of(t), :] = total.astype(bf16)
    outs = [
        remote(out_ref.at[rows_of(t)], out_ref.at[rows_of(t)], o_send.at[d], o_recv.at[d], (me, ts[d])) for d in t_order
    ]
    pump(len(pending))
    for copy in outs:
        copy.wait_recv()
    for copy in pages[-WINDOW:]:
        copy.wait_send()
    for copy in list(q_z.values()) + q_y + list(along_z.values()) + along_y + sums + outs:
        copy.wait_send()
    all_of(got, tag_sem).wait_send()
    all_of(part, part_sem).wait_send()
    all_of(lse, lse_sem).wait_send()
    moved_pages = comb_ref.at[pl.ds(SLOTS + CAP, (NDP - 1) * CAP)]
    pltpu.make_async_remote_copy(
        src_ref=moved_pages, dst_ref=moved_pages, send_sem=page_send.at[0], recv_sem=page_recv.at[0],
        device_id=(me, ts[1]), device_id_type=MESH,
    ).wait_recv()


def place_kernel(code_ref, comb_ref, proj_ref, new_ref, out_ref, sems, out_sem):
    copies = []
    for s in range(SLOTS):
        copies.append(pltpu.make_async_copy(comb_ref.at[code_ref[0, s]], new_ref.at[s], sems.at[s]))
        copies[-1].start()
    copies.append(pltpu.make_async_copy(proj_ref, out_ref, out_sem))
    copies[-1].start()
    for copy in copies:
        copy.wait()


def body(query, kv_pages, move_plan, move_count, block_table, seq_lens, out_weight):
    def in_hbm(x):
        return pltpu.with_memory_space_constraint(x, pltpu.HBM)

    kv = in_hbm(kv_pages.reshape(SLOTS, *PAGE))
    table = in_hbm(block_table)
    lens = in_hbm(seq_lens)
    dma = pltpu.SemaphoreType.DMA
    i32 = jnp.int32
    columns = out_weight.shape[1]
    seqs = NDP * SEQ_DEV
    comb, code, projected = pl.pallas_call(
        step_kernel,
        name="step",
        out_shape=[
            pltpu.VMEM((SLOTS + NDP * CAP, *PAGE), bf16),
            pltpu.VMEM((1, 128), i32),
            pltpu.VMEM((seqs, columns), bf16),
        ],
        in_specs=[sspec()] + [hspec()] * 6,
        out_specs=[vspec()] * 3,
        scratch_shapes=[
            pltpu.VMEM((3, 1, MOVES), i32),
            pltpu.SMEM((SEQ_DEV, BLOCKS), i32),
            pltpu.SMEM((SEQ_DEV,), i32),
            pltpu.VMEM((SEQ_DEV * HEADS, HD), bf16),
            pltpu.VMEM(out_weight.shape, bf16),
            pltpu.VMEM((SLOTS, *PAGE), bf16),
            pltpu.VMEM((NDP * CAP, *PAGE), bf16),
            pltpu.VMEM((NDP, 1, 128), i32),
            pltpu.VMEM((NDP, 1, 128), i32),
            pltpu.VMEM((NDP, SEQ_DEV * HEADS, HD), bf16),
            pltpu.VMEM((CAP, NDP, 1, 128), f32),
            pltpu.VMEM((CAP, NDP, 1, 128), f32),
            pltpu.VMEM((CAP, NDP, 1, 128), f32),
            pltpu.VMEM((NDP, CAP, HEADS, HD), bf16),
            pltpu.VMEM((NDP, 1, 128), f32),
            pltpu.VMEM((NDP, CAP, HEADS, HD), bf16),
            pltpu.VMEM((NDP, 1, 128), f32),
            pltpu.VMEM((SEQ_DEV + NDP * CAP, HEADS, 128), f32),
            pltpu.VMEM((SEQ_DEV * HEADS, HD), f32),
            pltpu.VMEM((SEQ_DEV, HEADS * HD), bf16),
            pltpu.VMEM((NDP, SEQ_DEV, HEADS * HD), bf16),
            pltpu.VMEM((seqs, columns), f32),
            pltpu.VMEM((NT, seqs // NT, columns), f32),
            dma((5,)), dma((2,)), dma((WINDOW,)), dma((1,)), dma((2,)), dma((2,)), dma((2,)),
            dma((NZ,)), dma((NZ,)), dma((NDP,)), dma((NDP,)),
            dma((NZ,)), dma((NZ,)), dma((NDP,)), dma((NDP,)),
            dma((NT,)), dma((NT,)), dma((NT,)), dma((NT,)),
        ],
        compiler_params=pltpu.CompilerParams(
            collective_id=0, has_side_effects=True, vmem_limit_bytes=VMEM_LIMIT
        ),
    )(move_count, in_hbm(jnp.transpose(move_plan, (1, 0, 2))), table, lens, in_hbm(query.reshape(SEQ_DEV * HEADS, HD)), in_hbm(out_weight), kv)
    new_pages, projected = pl.pallas_call(
        place_kernel,
        name="place",
        out_shape=[
            jax.ShapeDtypeStruct((SLOTS, *PAGE), bf16),
            jax.ShapeDtypeStruct((seqs, columns), bf16),
        ],
        in_specs=[sspec(), vspec(), vspec()],
        out_specs=[hspec(), hspec()],
        scratch_shapes=[dma((SLOTS,)), dma(())],
        compiler_params=pltpu.CompilerParams(vmem_limit_bytes=VMEM_LIMIT),
    )(code, comb, projected)
    return new_pages.reshape(kv_pages.shape), projected


def solution(mesh):
    placed = (
        P("dp", "tensor", None),
        P("dp", "tensor", None, None, None),
        P("dp", None, None),
        P("dp"),
        P("dp", None),
        P("dp"),
        P("tensor", "dp"),
    )
    return jax.shard_map(
        body,
        mesh=mesh,
        in_specs=placed,
        out_specs=(P("dp", "tensor", None, None, None), P(None, "dp")),
        check_vma=False,
    )
```

```python
import functools
import math

import jax
import jax.numpy as jnp
from jax import lax
from jax.experimental import pallas as pl
from jax.experimental.pallas import tpu as pltpu
from jax.sharding import PartitionSpec as P

HD = 128
BLOCK = 128
BLOCKS = 8
CAP = 2
SLOTS = 88
MOVES = 48
NY, NZ = 4, 8
NDP = NY * NZ
NT = 8
SEQ_DEV = 8
HEADS = 8
WINDOW = 12
TAG_LANE = SEQ_DEV * BLOCKS + SEQ_DEV
NEG = -1e30
SCALE = 1.0 / math.sqrt(HD)
MESH = pl.DeviceIdType.MESH
VMEM_LIMIT = 24 * 1024 * 1024
PAGE = (2, BLOCK, HD)
SHIFTS = [(dy, dz) for dy in range(NY) for dz in range(NZ)]
f32 = jnp.float32
bf16 = jnp.bfloat16


def far(shift):
    return min(shift[0], NY - shift[0]) + min(shift[1], NZ - shift[1])


def vspec():
    return pl.BlockSpec(memory_space=pltpu.VMEM)


def sspec():
    return pl.BlockSpec(memory_space=pltpu.SMEM)


def hspec():
    return pl.BlockSpec(memory_space=pltpu.HBM)


def step_kernel(
    count_ref, plan_hbm, table_hbm, lens_hbm, query_hbm, w_hbm, kv_ref,
    comb_ref, code_ref, out_ref,
    plan_ref, table_ref, lens_ref, query_ref, w_ref, local_ref, send_ref, tags_ref,
    got, qall, src_seq, src_end, arr_seq, part, lse, apart, alse, wide, mixed, att, gath, proj, red,
    in_sems, load_sem, page_send, page_recv, tag_sem, part_sem, lse_sem,
    qz_send, qz_recv, qy_send, qy_recv, z_send, z_recv, y_send, y_recv, r_send, r_recv, o_send, o_recv,
):
    me = lax.axis_index("dp")
    t = lax.axis_index("tensor")
    y, z = me // NZ, me % NZ
    zs = [lax.rem(z + d, NZ) for d in range(NZ)]
    ys = [lax.rem(y + d, NY) for d in range(NY)]
    ts = [lax.rem(t + d, NT) for d in range(NT)]
    bar = pltpu.get_barrier_semaphore()
    order = sorted([s for s in SHIFTS if s != (0, 0)], key=lambda s: -far(s))
    peers = [(ys[dy] * NZ + zs[dz], t) for dy, dz in order] + [(me, ts[d]) for d in range(1, NT)]
    for peer in peers:
        pl.semaphore_signal(bar, inc=1, device_id=peer, device_id_type=MESH)
    fetch = [
        pltpu.make_async_copy(a, b, in_sems.at[i])
        for i, (a, b) in enumerate(
            [(plan_hbm, plan_ref), (query_hbm, query_ref), (table_hbm, table_ref), (lens_hbm, lens_ref), (w_hbm, w_ref)]
        )
    ]
    load = pltpu.make_async_copy(kv_ref, local_ref, load_sem.at[0])
    keep = pltpu.make_async_copy(kv_ref, comb_ref.at[pl.ds(0, SLOTS)], load_sem.at[1])
    for copy in fetch[:4] + [load]:
        copy.start()

    i32 = jnp.int32
    for copy in fetch[:4]:
        copy.wait()

    def iota(shape, axis):
        return lax.broadcasted_iota(i32, shape, axis)

    plan = [jnp.broadcast_to(plan_ref[r], (MOVES, MOVES)) for r in range(3)]
    down, across = iota((MOVES, MOVES), 0), iota((MOVES, MOVES), 1)
    target = jnp.sum(jnp.where(down == across, plan[1], 0), axis=1, keepdims=True)
    before = (target == plan[1]) & (down < across) & (down < count_ref[0])
    rank = jnp.sum(jnp.where(before, 1, 0), axis=0, keepdims=True)
    goes = plan_ref[1]
    shift = (((goes >> 3) - y) & (NY - 1)) * NZ + ((goes - z) & (NZ - 1))
    row = jnp.where(iota((1, MOVES), 1) < count_ref[0], shift * CAP + rank, -1)
    lane = iota((NDP, 128), 1)
    lane1 = iota((1, 128), 1)
    meta = jnp.full((1, 128), -2, i32)
    for s in range(SEQ_DEV):
        for b in range(BLOCKS):
            meta = jnp.where(lane1 == s * BLOCKS + b, table_ref[s, b], meta)
        meta = jnp.where(lane1 == SEQ_DEV * BLOCKS + s, lens_ref[s], meta)
    tags = jnp.broadcast_to(meta, (NDP, 128))
    source = []
    for c in range(CAP):
        hit = jnp.broadcast_to(row, (NDP, MOVES)) == iota((NDP, MOVES), 0) * CAP + c
        source.append(
            jnp.sum(jnp.where(hit, jnp.broadcast_to(plan_ref[0], (NDP, MOVES)), 0), axis=1, keepdims=True)
        )
        slot = jnp.sum(jnp.where(hit, jnp.broadcast_to(plan_ref[2], (NDP, MOVES)) + 1, 0), axis=1, keepdims=True) - 1
        tags = jnp.where(lane == TAG_LANE + c, slot, tags)
    tags_ref[...] = tags.reshape(NDP, 1, 128)
    load.wait()
    keep.start()
    fetch[4].start()

    def take(c, k):
        send_ref[k * CAP + c] = local_ref[source[c][k, 0]]

    for c, (dy, dz) in [(c, s) for c in range(CAP) for s in order]:
        take(c, dy * NZ + dz)
    for c in range(CAP):
        take(c, 0)
    pl.semaphore_wait(bar, len(peers))

    def remote(src, dst, send, recv, device):
        copy = pltpu.make_async_remote_copy(
            src_ref=src, dst_ref=dst, send_sem=send, recv_sem=recv, device_id=device, device_id_type=MESH
        )
        copy.start()
        return copy

    def to(shift):
        return (ys[shift[0]] * NZ + zs[shift[1]], t)

    def at(shift):
        return shift[0] * NZ + shift[1]

    pages = []
    pending = [(c, s) for c in range(CAP) for s in order]

    def pump(n):
        for _ in range(n):
            i = len(pages)
            if i >= len(pending):
                return
            if i >= WINDOW:
                pages[i - WINDOW].wait_send()
            c, s = pending[i]
            row = at(s) * CAP + c
            pages.append(
                remote(send_ref.at[row], comb_ref.at[SLOTS + row], page_send.at[i % WINDOW], page_recv.at[0], to(s))
            )

    relays = {2: (1, 2), 6: (7,)}

    def gather_start(own_ref, buf, zsend, zrecv, ysend, yrecv, sign):
        along_z = {}
        for d in (2, 6, 1, 7):
            e = d * sign % NZ
            along_z[e] = remote(own_ref, buf.at[me], zsend.at[e], zrecv.at[e], (y * NZ + zs[e], t))
        along_y = [
            remote(own_ref, buf.at[me], ysend.at[d], yrecv.at[d], (ys[d] * NZ + z, t)) for d in (2, 1, 3)
        ]
        buf[me] = own_ref[...]
        return along_z, along_y

    def gather_forward(along_z, along_y, buf, zsend, zrecv, ysend, yrecv, sign, pumps):
        for d in (2, 6, 1, 7, 3, 5, 4):
            e = d * sign % NZ
            along_z[e].wait_recv()
            held = y * NZ + lax.rem(z - e + NZ, NZ)
            for step in relays.get(d, ()):
                there = (d + step) * sign % NZ
                along_z[there] = remote(
                    buf.at[held], buf.at[held], zsend.at[there], zrecv.at[there],
                    (y * NZ + zs[step * sign % NZ], t),
                )
            for d_y in (2, 1, 3):
                n = e * NY + d_y
                along_y.append(
                    remote(buf.at[held], buf.at[held], ysend.at[n], yrecv.at[n], (ys[d_y] * NZ + z, t))
                )
            pump(pumps)

    q_z, q_y = gather_start(query_ref, qall, qz_send, qz_recv, qy_send, qy_recv, 1)
    small = []
    for s in order:
        small.append(remote(tags_ref.at[at(s)], got.at[at(s)], tag_sem.at[0], tag_sem.at[1], to(s)))
    got[0] = tags_ref[0]
    pump(WINDOW)
    comb_ref[SLOTS : SLOTS + CAP] = send_ref[0:CAP]
    gather_forward(q_z, q_y, qall, qz_send, qz_recv, qy_send, qy_recv, 1, 1)

    def all_of(buf, sems):
        return pltpu.make_async_remote_copy(
            src_ref=buf.at[pl.ds(1, NDP - 1)],
            dst_ref=buf.at[pl.ds(1, NDP - 1)],
            send_sem=sems.at[0],
            recv_sem=sems.at[1],
            device_id=(me, ts[1]),
            device_id_type=MESH,
        )

    all_of(got, tag_sem).wait_recv()
    lane_f = lane.astype(f32)
    first = lane < SEQ_DEV * BLOCKS
    seq_f = (lane // BLOCKS).astype(f32)
    block_f = (lane % BLOCKS).astype(f32)
    device_f = lax.broadcasted_iota(jnp.int32, (NDP, 128), 0).astype(f32)
    mine = got[0]
    moved = jnp.zeros((1, 128), f32)
    code = lane1.astype(f32)
    sent_tags = tags_ref[...].reshape(NDP, 128)
    got_tags = got[...].reshape(NDP, 128)
    tables = jnp.concatenate([got[at(((NY - dy) % NY, (NZ - dz) % NZ))] for dy, dz in SHIFTS], axis=0)

    def spread(column):
        return jnp.broadcast_to(column, (NDP, 128)).reshape(NDP, 1, 128)

    for c in range(CAP):
        tag = sent_tags[:, TAG_LANE + c : TAG_LANE + c + 1]
        hit = (tables == tag) & first & (tag >= 0)
        found = jnp.sum(jnp.where(hit, 1.0, 0.0), axis=1, keepdims=True)
        seq = jnp.sum(jnp.where(hit, seq_f, 0.0), axis=1, keepdims=True)
        block = jnp.sum(jnp.where(hit, block_f, 0.0), axis=1, keepdims=True)
        ends = jnp.sum(
            jnp.where(lane_f == seq + SEQ_DEV * BLOCKS, tables.astype(f32), 0.0), axis=1, keepdims=True
        )
        src_seq[c] = spread(jnp.where(found > 0, seq, -1.0))
        src_end[c] = spread(ends - block * BLOCK)
        tag = got_tags[:, TAG_LANE + c : TAG_LANE + c + 1]
        hit = (mine == tag) & first & (tag >= 0)
        found = jnp.sum(jnp.where(hit, 1.0, 0.0), axis=1, keepdims=True)
        seq = jnp.sum(jnp.where(hit, seq_f, 0.0), axis=1, keepdims=True)
        arr_seq[c] = spread(jnp.where(found > 0, seq, -1.0))
        moved = jnp.maximum(moved, jnp.max(jnp.where(hit, 1.0, 0.0), axis=0, keepdims=True))
        code = code + jnp.sum(
            jnp.where(lane == tag, device_f * CAP + (SLOTS + c) - lane_f, 0.0), axis=0, keepdims=True
        )
    code_ref[...] = code.astype(jnp.int32)
    pump(2)

    keep.wait()
    position = lax.broadcasted_iota(jnp.int32, (HEADS, BLOCKS * BLOCK), 1)
    kept_o = []
    kept_lse = []
    for s in range(SEQ_DEV):
        index = [table_ref[s, b] for b in range(BLOCKS)]
        keys = jnp.concatenate([local_ref[i, 0] for i in index], axis=0)
        scores = lax.dot_general(
            query_ref[s * HEADS : (s + 1) * HEADS, :], keys, (((1,), (1,)), ((), ())), preferred_element_type=f32
        ) * SCALE
        gone = jnp.concatenate(
            [jnp.broadcast_to(moved[:, s * BLOCKS + b : s * BLOCKS + b + 1], (1, BLOCK)) for b in range(BLOCKS)], axis=1
        )
        scores = jnp.where((position < lens_ref[s]) & (gone == 0), scores, NEG)
        largest = jnp.max(scores, axis=1, keepdims=True)
        expo = jnp.exp(scores - largest)
        total = jnp.sum(expo, axis=1, keepdims=True)
        values = jnp.concatenate([local_ref[i, 1] for i in index], axis=0)
        mixed[s * HEADS : (s + 1) * HEADS, :] = (
            jnp.dot(expo.astype(bf16), values, preferred_element_type=f32) / total
        )
        wide[s] = jnp.broadcast_to(largest + jnp.log(total), (HEADS, 128))
        if s % 2:
            pump(1)

    for copy in q_y:
        copy.wait_recv()
    lane8 = lax.broadcasted_iota(jnp.int32, (HEADS, 128), 1)
    row8 = lax.broadcasted_iota(jnp.int32, (HEADS, 128), 0)
    lane8_f = lane8.astype(f32)

    def rows8(ref, c, k):
        return jnp.broadcast_to(ref[c, k], (HEADS, 128))

    def partial(k, carry):
        dy, dz = k // NZ, lax.rem(k, NZ)
        owner = lax.rem(y + dy, NY) * NZ + lax.rem(z + dz, NZ)
        asked = qall[owner]
        keys = jnp.concatenate([send_ref[k * CAP + c, 0] for c in range(CAP)], axis=0)
        every = lax.dot_general(asked, keys, (((1,), (1,)), ((), ())), preferred_element_type=f32) * SCALE
        row = jnp.zeros((1, 128), f32)
        for c in range(CAP):
            seq = rows8(src_seq, c, k)
            scores = jnp.full((HEADS, BLOCK), NEG, f32)
            for s in range(SEQ_DEV):
                scores = jnp.where(
                    seq == s, every[s * HEADS : (s + 1) * HEADS, c * BLOCK : (c + 1) * BLOCK], scores
                )
            scores = jnp.where(lane8_f < rows8(src_end, c, k), scores, NEG)
            largest = jnp.max(scores, axis=1, keepdims=True)
            expo = jnp.exp(scores - largest)
            total = jnp.sum(expo, axis=1, keepdims=True)
            o = jnp.dot(expo.astype(bf16), send_ref[k * CAP + c, 1], preferred_element_type=f32) / total
            part[k, c] = jnp.where(seq >= 0, o, 0.0).astype(bf16)
            weight = jnp.where(seq >= 0, largest + jnp.log(total), NEG)
            row = row + jnp.sum(jnp.where(lane8 == row8 + c * HEADS, weight, 0.0), axis=0, keepdims=True)
        lse[k] = row
        return carry

    for g in range(4):
        lax.fori_loop(g * NZ, (g + 1) * NZ, partial, 0, unroll=4)
        for dz in range(NZ):
            if (g, dz) != (0, 0):
                k = at((g, dz))
                small.append(remote(part.at[k], apart.at[k], part_sem.at[0], part_sem.at[1], to((g, dz))))
                small.append(remote(lse.at[k], alse.at[k], lse_sem.at[0], lse_sem.at[1], to((g, dz))))
        pump(2)
    apart[0] = part[0]
    alse[0] = lse[0]
    pump(3)
    all_of(apart, part_sem).wait_recv()
    all_of(alse, lse_sem).wait_recv()

    def widen(k, tops):
        tops = list(tops)
        for c in range(CAP):
            column = jnp.sum(
                jnp.where(lane8 == row8 + c * HEADS, jnp.broadcast_to(alse[k], (HEADS, 128)), 0.0),
                axis=1,
                keepdims=True,
            )
            full = jnp.broadcast_to(column, (HEADS, 128))
            wide[SEQ_DEV + k * CAP + c] = full
            seq = rows8(arr_seq, c, k)
            for s in range(SEQ_DEV):
                tops[s] = jnp.where(seq == s, jnp.maximum(tops[s], full), tops[s])
        return tuple(tops)

    tops = lax.fori_loop(0, NDP, widen, tuple(wide[s] for s in range(SEQ_DEV)), unroll=4)
    start = []
    for s in range(SEQ_DEV):
        w = jnp.exp(wide[s] - tops[s])
        start.append((w, w * mixed[s * HEADS : (s + 1) * HEADS, :]))

    def merge(k, sums):
        dens, nums = list(sums[0]), list(sums[1])
        for c in range(CAP):
            seq = rows8(arr_seq, c, k)
            top = jnp.zeros((HEADS, 128), f32)
            for s in range(SEQ_DEV):
                top = jnp.where(seq == s, tops[s], top)
            w = jnp.exp(wide[SEQ_DEV + k * CAP + c] - top)
            o = w * apart[k, c].astype(f32)
            for s in range(SEQ_DEV):
                dens[s] = jnp.where(seq == s, dens[s] + w, dens[s])
                nums[s] = jnp.where(seq == s, nums[s] + o, nums[s])
        return tuple(dens), tuple(nums)

    dens, nums = lax.fori_loop(
        0, NDP, merge, (tuple(a for a, _ in start), tuple(b for _, b in start)), unroll=4
    )
    for s in range(SEQ_DEV):
        mixed[s * HEADS : (s + 1) * HEADS, :] = nums[s] / dens[s]
    att[...] = jnp.concatenate(
        [mixed[pl.ds(h, SEQ_DEV, stride=HEADS), :] for h in range(HEADS)], axis=1
    ).astype(bf16)

    along_z, along_y = gather_start(att, gath, z_send, z_recv, y_send, y_recv, -1)
    pump(4)
    gather_forward(along_z, along_y, gath, z_send, z_recv, y_send, y_recv, -1, 1)
    pump(2)
    for copy in along_y:
        copy.wait_recv()
    fetch[4].wait()
    rows = gath[...].reshape(NDP * SEQ_DEV, HEADS * HD)
    proj[...] = jnp.dot(rows, w_ref[...], preferred_element_type=f32)
    chunk = NDP * SEQ_DEV // NT
    t_order = (4, 5, 3, 2, 6, 1, 7)

    def rows_of(i):
        return pl.ds(pl.multiple_of(i * chunk, chunk), chunk)

    sums = [remote(proj.at[rows_of(ts[d])], red.at[d], r_send.at[d], r_recv.at[d], (me, ts[d])) for d in t_order]
    pump(2)
    total = proj[rows_of(t), :]
    for copy in sums:
        copy.wait_recv()
    for d in range(1, NT):
        total = total + red[d]
    out_ref[rows_of(t), :] = total.astype(bf16)
    outs = [
        remote(out_ref.at[rows_of(t)], out_ref.at[rows_of(t)], o_send.at[d], o_recv.at[d], (me, ts[d])) for d in t_order
    ]
    pump(len(pending))
    for copy in outs:
        copy.wait_recv()
    for copy in pages[-WINDOW:]:
        copy.wait_send()
    for copy in list(q_z.values()) + q_y + list(along_z.values()) + along_y + sums + outs:
        copy.wait_send()
    all_of(got, tag_sem).wait_send()
    all_of(part, part_sem).wait_send()
    all_of(lse, lse_sem).wait_send()
    moved_pages = comb_ref.at[pl.ds(SLOTS + CAP, (NDP - 1) * CAP)]
    pltpu.make_async_remote_copy(
        src_ref=moved_pages, dst_ref=moved_pages, send_sem=page_send.at[0], recv_sem=page_recv.at[0],
        device_id=(me, ts[1]), device_id_type=MESH,
    ).wait_recv()


def place_kernel(code_ref, comb_ref, proj_ref, new_ref, out_ref, sems, out_sem):
    copies = []
    for s in range(SLOTS):
        copies.append(pltpu.make_async_copy(comb_ref.at[code_ref[0, s]], new_ref.at[s], sems.at[s]))
        copies[-1].start()
    copies.append(pltpu.make_async_copy(proj_ref, out_ref, out_sem))
    copies[-1].start()
    for copy in copies:
        copy.wait()


def body(query, kv_pages, move_plan, move_count, block_table, seq_lens, out_weight):
    def in_hbm(x):
        return pltpu.with_memory_space_constraint(x, pltpu.HBM)

    kv = in_hbm(kv_pages.reshape(SLOTS, *PAGE))
    table = in_hbm(block_table)
    lens = in_hbm(seq_lens)
    dma = pltpu.SemaphoreType.DMA
    i32 = jnp.int32
    columns = out_weight.shape[1]
    seqs = NDP * SEQ_DEV
    comb, code, projected = pl.pallas_call(
        step_kernel,
        name="step",
        out_shape=[
            pltpu.VMEM((SLOTS + NDP * CAP, *PAGE), bf16),
            pltpu.VMEM((1, 128), i32),
            pltpu.VMEM((seqs, columns), bf16),
        ],
        in_specs=[sspec()] + [hspec()] * 6,
        out_specs=[vspec()] * 3,
        scratch_shapes=[
            pltpu.VMEM((3, 1, MOVES), i32),
            pltpu.SMEM((SEQ_DEV, BLOCKS), i32),
            pltpu.SMEM((SEQ_DEV,), i32),
            pltpu.VMEM((SEQ_DEV * HEADS, HD), bf16),
            pltpu.VMEM(out_weight.shape, bf16),
            pltpu.VMEM((SLOTS, *PAGE), bf16),
            pltpu.VMEM((NDP * CAP, *PAGE), bf16),
            pltpu.VMEM((NDP, 1, 128), i32),
            pltpu.VMEM((NDP, 1, 128), i32),
            pltpu.VMEM((NDP, SEQ_DEV * HEADS, HD), bf16),
            pltpu.VMEM((CAP, NDP, 1, 128), f32),
            pltpu.VMEM((CAP, NDP, 1, 128), f32),
            pltpu.VMEM((CAP, NDP, 1, 128), f32),
            pltpu.VMEM((NDP, CAP, HEADS, HD), bf16),
            pltpu.VMEM((NDP, 1, 128), f32),
            pltpu.VMEM((NDP, CAP, HEADS, HD), bf16),
            pltpu.VMEM((NDP, 1, 128), f32),
            pltpu.VMEM((SEQ_DEV + NDP * CAP, HEADS, 128), f32),
            pltpu.VMEM((SEQ_DEV * HEADS, HD), f32),
            pltpu.VMEM((SEQ_DEV, HEADS * HD), bf16),
            pltpu.VMEM((NDP, SEQ_DEV, HEADS * HD), bf16),
            pltpu.VMEM((seqs, columns), f32),
            pltpu.VMEM((NT, seqs // NT, columns), f32),
            dma((5,)), dma((2,)), dma((WINDOW,)), dma((1,)), dma((2,)), dma((2,)), dma((2,)),
            dma((NZ,)), dma((NZ,)), dma((NDP,)), dma((NDP,)),
            dma((NZ,)), dma((NZ,)), dma((NDP,)), dma((NDP,)),
            dma((NT,)), dma((NT,)), dma((NT,)), dma((NT,)),
        ],
        compiler_params=pltpu.CompilerParams(
            collective_id=0, has_side_effects=True, vmem_limit_bytes=VMEM_LIMIT
        ),
    )(move_count, in_hbm(jnp.transpose(move_plan, (1, 0, 2))), table, lens, in_hbm(query.reshape(SEQ_DEV * HEADS, HD)), in_hbm(out_weight), kv)
    new_pages, projected = pl.pallas_call(
        place_kernel,
        name="place",
        out_shape=[
            jax.ShapeDtypeStruct((SLOTS, *PAGE), bf16),
            jax.ShapeDtypeStruct((seqs, columns), bf16),
        ],
        in_specs=[sspec(), vspec(), vspec()],
        out_specs=[hspec(), hspec()],
        scratch_shapes=[dma((SLOTS,)), dma(())],
        compiler_params=pltpu.CompilerParams(vmem_limit_bytes=VMEM_LIMIT),
    )(code, comb, projected)
    return new_pages.reshape(kv_pages.shape), projected


def solution(mesh):
    placed = (
        P("dp", "tensor", None),
        P("dp", "tensor", None, None, None),
        P("dp", None, None),
        P("dp"),
        P("dp", None),
        P("dp"),
        P("tensor", "dp"),
    )
    return jax.shard_map(
        body,
        mesh=mesh,
        in_specs=placed,
        out_specs=(P("dp", "tensor", None, None, None), P(None, "dp")),
        check_vma=False,
    )
```
